256 devices in a mesh: dp: 32 (over y, x, core), seq: 8 (over z).
Axes of the slice: x: 4, y: 4, z: 8, core: 2. Of those that a mesh axis runs over, the one named last changes fastest.
Arguments:
- query_rows: bfloat16 [32, 1024, 3072], P('dp', 'seq'), may hold values from -6 to 6
- key_rows: bfloat16 [32, 1024, 3072], P('dp', 'seq'), may hold values from -6 to 6
- value_rows: bfloat16 [32, 1024, 3072], P('dp', 'seq'), may hold values from -6 to 6
- out_grad: bfloat16 [32, 1024, 6144], P('dp', 'seq'), may hold values from -54 to 54
- clip_lengths: int32 [32, 4], P('dp'), may hold values from 1 to 512, 1024 in all within a row
- out_weight: bfloat16 [3072, 6144], P('seq'), may hold values from -0.109375 to 0.109375
- query_gain: float32 [128], replicated, may hold values from 0.1 to 1.9
- key_gain: float32 [128], replicated, may hold values from 0.1 to 1.9
Outputs:
- query_grad: bfloat16 [32, 1024, 3072], P('dp', 'seq')
- key_grad: bfloat16 [32, 1024, 3072], P('dp', 'seq')
- value_grad: bfloat16 [32, 1024, 3072], P('dp', 'seq')
- weight_grad: float32 [3072, 6144], P('seq', 'dp')
- querygain_grad: float32 [128], replicated
- keygain_grad: float32 [128], replicated
- grad_norm: float32 [], replicated
The draws below stay inside these ranges and needn't reach their ends.
Inputs may be any that keep to these rules, and one draw needn't show every extreme that they name: `clip_lengths`: the token counts of each group's clips sum to 1024.
All inputs are finite; a program needn't handle non-finite values.
Results may differ from the reference program's by a relative error of at most 0.015.
Values may be sent and summed in bfloat16 or wider, within the bound.
A program may use at most 128 MiB of HBM per device.

```python
import math
import jax
import jax.numpy as jnp
import numpy as np
from jax import lax

D = 6144
HEAD_DIM = 128
CLIPS = 4
GROUPS = 32
SEQ_LEN = 1024
INNER = 3072
MAX_NORM = 768


def draw_out_grad(key, part):
    first = jax.random.fold_in(key, 0)
    second = jax.random.fold_in(key, 1)
    fifth = jax.random.fold_in(key, 4)
    row_scale = jnp.exp(jax.random.uniform(first, (GROUPS, SEQ_LEN, 1), jnp.float32, -1.2, 1.1))
    ramp = 0.5 + jnp.arange(D, dtype=jnp.float32) / (D - 1)
    column_scale = ramp * jnp.exp(jax.random.uniform(second, (D,), jnp.float32, -1.2, 1.1))
    base = jax.random.truncated_normal(fifth, -4.0, 4.0, (GROUPS, SEQ_LEN, D), jnp.float32)
    return (row_scale * column_scale * base).astype(jnp.bfloat16)


def block_scale(rng, dims, shards, smallest, top_value):
    loudness = 1.0
    for dim, blocks in shards:
        steps = jax.random.uniform(jax.random.fold_in(jax.random.fold_in(rng, 6), dim), (blocks,), jnp.float32, smallest / len(shards), top_value / len(shards))
        loudness = loudness * jnp.repeat(jnp.exp(steps), dims[dim] // blocks).reshape((-1,) + (1,) * (len(dims) - 1 - dim))
    return loudness


def length_profile(number_of, total, most, lean):
    loads = [(1 << 20) // math.isqrt(standing ** lean) + 1 for standing in range(2, number_of + 1)]
    rest, holding = total - most - (number_of - 1), [1] * (number_of - 1)
    while rest > 0:
        free = [i for i in range(number_of - 1) if holding[i] < most]
        pool, remaining = sum([loads[i] for i in free]), rest
        for i in free:
            addition = min(most - holding[i], max(1, remaining * loads[i] // pool), rest)
            holding[i] = holding[i] + addition
            rest = rest - addition
    return np.array([most] + holding)


def ragged_sizes(own_key, amount, total, bound, slope):
    if amount == 2:
        one = jax.random.randint(own_key, (), max(1, total - bound), min(bound, total - 1) + 1)
        return jnp.stack([one, total - one])
    sizes = jnp.asarray(length_profile(amount, total, bound, slope), jnp.int32)
    couples = (amount - 1) // 2
    giver, receiver = sizes[1:1 + 2 * couples:2], sizes[2:2 + 2 * couples:2]
    room = jnp.minimum(giver - 1, bound - receiver)
    passed = jax.random.randint(jax.random.fold_in(own_key, 1), (couples,), 0, 1 << 20) % (room + 1)
    sizes = sizes.at[1:1 + 2 * couples:2].set(giver - passed).at[2:2 + 2 * couples:2].set(receiver + passed)
    return sizes[jax.random.permutation(jax.random.fold_in(own_key, 2), amount)]


def bell_draw(own_key, shape, scale, limit, cuts=(), held_as=jnp.bfloat16):
    values = jax.random.normal(own_key, shape, jnp.float32) * scale
    if len(cuts) > 0:
        values = block_scale(own_key, shape, cuts, -0.22, 0.18) * values
    return jnp.clip(values, min=-limit, max=limit).astype(held_as)


def setup_inputs(seed: int = 0) -> dict:
    splits = jax.random.split(jax.random.key(seed), 9)
    return {
        "query_rows": bell_draw(splits[0], (GROUPS, SEQ_LEN, INNER), 1.0, 6.0, ((0, 32), (1, 8))),
        "key_rows": bell_draw(splits[1], (GROUPS, SEQ_LEN, INNER), 1.0, 6.0, ((0, 32), (1, 8))),
        "value_rows": bell_draw(splits[2], (GROUPS, SEQ_LEN, INNER), 1.0, 6.0, ((0, 32), (1, 8))),
        "out_grad": draw_out_grad(jax.random.fold_in(splits[8], 71), 0),
        "clip_lengths": jax.vmap(lambda own: ragged_sizes(own, CLIPS, SEQ_LEN, SEQ_LEN // 2, 2))(jax.random.split(splits[4], GROUPS)).reshape((GROUPS, CLIPS)).astype(jnp.int32),
        "out_weight": bell_draw(splits[5], (INNER, D), INNER ** -0.5, 0.109375, ((0, 8),)),
        "query_gain": jnp.clip(1.0 + 0.18 * jax.random.normal(splits[6], (HEAD_DIM,), jnp.float32), 0.1, 1.9),
        "key_gain": jnp.clip(1.0 + 0.18 * jax.random.normal(splits[7], (HEAD_DIM,), jnp.float32), 0.1, 1.9),
    }


EPS = 1e-06

def segment_ids(lengths, total):
    ends = jnp.cumsum(lengths.astype(jnp.int32))
    places = jnp.arange(total, dtype=jnp.int32)
    return lax.optimization_barrier(jnp.sum((places[:, None] >= ends[None, :]).astype(jnp.int32), axis=1)).astype(jnp.int32)

def norm_rows(rows, gain):
    wide = rows.astype(jnp.float32)
    inverse = lax.rsqrt(lax.optimization_barrier(jnp.mean(wide * wide, axis=-1, keepdims=True)) + EPS)
    unit = wide * inverse
    return (unit, inverse, (unit * gain).astype(jnp.bfloat16))

def norm_back(unit, inverse, gain, d_norm):
    gain_part = lax.optimization_barrier(jnp.sum(unit * d_norm, axis=(0, 1)))
    d_unit = d_norm * gain
    d_rows = inverse * (d_unit - unit * lax.optimization_barrier(jnp.mean(unit * d_unit, axis=-1, keepdims=True)))
    return (d_rows.astype(jnp.bfloat16), gain_part)

def one_group(query, keys, values, d_out, lengths, out_weight, query_gain, key_gain):
    total = query.shape[0]
    heads = query.shape[1] // HEAD_DIM
    scale = HEAD_DIM ** (-0.5)
    query3 = query.reshape(total, heads, HEAD_DIM)
    keys3 = keys.reshape(total, heads, HEAD_DIM)
    values3 = values.reshape(total, heads, HEAD_DIM).astype(jnp.float32)
    seg = segment_ids(lengths, total)
    same = seg[:, None] == seg[None, :]
    q_unit, q_inv, q_norm = norm_rows(query3, query_gain)
    k_unit, k_inv, k_norm = norm_rows(keys3, key_gain)
    scores = jnp.einsum('qhd,khd->hqk', q_norm.astype(jnp.float32), k_norm.astype(jnp.float32)) * scale
    expo = jnp.where(same[None], jnp.exp(scores), 0.0)
    probs = (expo / lax.optimization_barrier(jnp.sum(expo, axis=-1, keepdims=True))).astype(jnp.bfloat16)
    probs32 = probs.astype(jnp.float32)
    attn_out = jnp.einsum('hqk,khd->qhd', probs32, values3).astype(jnp.bfloat16)
    attn_flat = attn_out.reshape(total, heads * HEAD_DIM)
    weight_part = jnp.dot(attn_flat.T, d_out, preferred_element_type=jnp.float32)
    d_attn = jnp.dot(d_out, out_weight.T, preferred_element_type=jnp.float32).astype(jnp.bfloat16)
    d_attn32 = d_attn.reshape(total, heads, HEAD_DIM).astype(jnp.float32)
    d_probs = jnp.einsum('qhd,khd->hqk', d_attn32, values3)
    row_sum = lax.optimization_barrier(jnp.sum(probs32 * d_probs, axis=-1, keepdims=True))
    d_scores = (probs32 * (d_probs - row_sum) * scale).astype(jnp.bfloat16).astype(jnp.float32)
    value_grad = jnp.einsum('hqk,qhd->khd', probs32, d_attn32).astype(jnp.bfloat16)
    d_qnorm = jnp.einsum('hqk,khd->qhd', d_scores, k_norm.astype(jnp.float32))
    d_knorm = jnp.einsum('hqk,qhd->khd', d_scores, q_norm.astype(jnp.float32))
    query_grad, q_gain_part = norm_back(q_unit, q_inv, query_gain, d_qnorm)
    key_grad, k_gain_part = norm_back(k_unit, k_inv, key_gain, d_knorm)
    width = heads * HEAD_DIM
    return (query_grad.reshape(total, width), key_grad.reshape(total, width), value_grad.reshape(total, width), weight_part, q_gain_part, k_gain_part)

def reference(query_rows, key_rows, value_rows, out_grad, clip_lengths, out_weight, query_gain, key_gain):

    def step(carry, items):
        weight_sum, q_gain_sum, k_gain_sum = carry
        query, keys, values, d_out, lengths = items
        q_grad, k_grad, v_grad, weight_part, q_part, k_part = one_group(query, keys, values, d_out, lengths, out_weight, query_gain, key_gain)
        return ((weight_sum + weight_part, q_gain_sum + q_part, k_gain_sum + k_part), (q_grad, k_grad, v_grad))
    start = (jnp.zeros(out_weight.shape, jnp.float32), jnp.zeros((HEAD_DIM,), jnp.float32), jnp.zeros((HEAD_DIM,), jnp.float32))
    (weight_raw, qgain_raw, kgain_raw), (query_grad, key_grad, value_grad) = lax.scan(step, start, (query_rows, key_rows, value_rows, out_grad, clip_lengths))
    squares = jnp.sum(weight_raw * weight_raw) + jnp.sum(qgain_raw * qgain_raw) + jnp.sum(kgain_raw * kgain_raw)
    grad_norm = jnp.sqrt(squares)
    factor = jnp.minimum(jnp.float32(1.0), MAX_NORM / (grad_norm + EPS))
    return (query_grad, key_grad, value_grad, weight_raw * factor, qgain_raw * factor, kgain_raw * factor, grad_norm)
```

```python
import functools

import jax
import jax.numpy as jnp
from jax import lax
from jax.experimental import pallas as pl
from jax.experimental.pallas import tpu as pltpu
from jax.sharding import Mesh
from jax.sharding import PartitionSpec as P

HEAD_DIM = 128
MAX_NORM = 768
EPS = 1e-06
DP = ("dp_0", "dp_1", "dp_2")
MESH = pl.DeviceIdType.MESH
F32 = jnp.float32
BF16 = jnp.bfloat16
NN = (((1,), (0,)), ((), ()))
NT = (((1,), (1,)), ((), ()))
SUBS = 2


def dot(a, b, dims=NN):
    return lax.dot_general(a, b, dims, preferred_element_type=F32)


def seg_of(places, ends_ref):
    seg = jnp.zeros(places.shape, jnp.int32)
    for c in range(ends_ref.shape[0]):
        seg = seg + (places >= ends_ref[c]).astype(jnp.int32)
    return seg


def attention_kernel(
    n,
    q_hbm,
    k_hbm,
    v_hbm,
    do_hbm,
    w_hbm,
    ends_ref,
    qg_ref,
    kg_ref,
    dq_out,
    dk_out,
    dv_out,
    wp_out,
    gain_out,
    qkv,
    kn,
    knt,
    vt,
    do_all,
    w,
    wacc,
    dkt,
    dvt,
    datt,
    attnt,
    dqs,
    qkv_send,
    qkv_recv,
    ag_send,
    ag_recv,
    dq_send,
    dq_recv,
    own_sem,
):
    me = lax.axis_index("seq")
    core = lax.axis_index("dp_2")
    sign = 1 - 2 * core
    tokens = q_hbm.shape[0]
    total = tokens * n
    width = q_hbm.shape[1] // n
    heads = width // HEAD_DIM
    model = do_hbm.shape[1]
    scale = HEAD_DIM ** (-0.5)
    half = tokens // SUBS
    up = lax.rem(me + sign + n, n)
    down = lax.rem(me - sign + n, n)
    a_steps = n // 2
    b_steps = n - 1 - a_steps

    def columns(index):
        return pl.ds(pl.multiple_of(index * width, width), width)

    def rows_of(index):
        return pl.ds(pl.multiple_of(index * tokens, tokens), tokens)

    def peer(d):
        return lax.rem(me + d, n)

    barrier = pltpu.get_barrier_semaphore()
    for d in range(1, n):
        pl.semaphore_signal(barrier, inc=1, device_id={"seq": peer(d)}, device_id_type=MESH)

    w_copy = pltpu.make_async_copy(w_hbm, w, own_sem.at[4])
    do_copy = pltpu.make_async_copy(do_hbm, do_all.at[me], own_sem.at[3])
    own_copies = [
        pltpu.make_async_copy(ref.at[:, columns(me)], qkv.at[i, rows_of(me)], own_sem.at[i])
        for i, ref in enumerate((q_hbm, k_hbm, v_hbm))
    ]
    for copy in own_copies + [do_copy, w_copy]:
        copy.start()
    pl.semaphore_wait(barrier, n - 1)

    def qkv_copy(i, ref, d):
        to = peer(d)
        return pltpu.make_async_remote_copy(
            src_ref=ref.at[:, columns(to)],
            dst_ref=qkv.at[i, rows_of(me)],
            send_sem=qkv_send.at[i, d],
            recv_sem=qkv_recv.at[i, me],
            device_id={"seq": to},
            device_id_type=MESH,
        )

    def qkv_arrival(i, ref, d):
        source = peer(d)
        return pltpu.make_async_remote_copy(
            src_ref=ref.at[:, columns(me)],
            dst_ref=qkv.at[i, rows_of(source)],
            send_sem=qkv_send.at[i, d],
            recv_sem=qkv_recv.at[i, source],
            device_id={"seq": source},
            device_id_type=MESH,
        )

    order = [4, 3, 5, 2, 6, 1, 7] if n == 8 else list(range(1, n))
    arrays = ((1, k_hbm), (2, v_hbm), (0, q_hbm))
    for i, ref in arrays:
        for d in order:
            qkv_copy(i, ref, d).start()

    def ring(direction, step, sub, block, to, source=None):
        piece = pl.ds(sub * half, half)
        return pltpu.make_async_remote_copy(
            src_ref=do_all.at[block, piece] if source is None else source.at[piece],
            dst_ref=do_all.at[block, piece],
            send_sem=ag_send.at[direction, step, sub],
            recv_sem=ag_recv.at[block, sub],
            device_id={"seq": to},
            device_id_type=MESH,
        )

    for sub in range(SUBS):
        ring(0, 0, sub, me, up, do_hbm).start()
        ring(1, 0, sub, me, down, do_hbm).start()

    dkt[...] = jnp.zeros(dkt.shape, F32)
    dvt[...] = jnp.zeros(dvt.shape, F32)
    gain_out[...] = jnp.zeros(gain_out.shape, F32)

    def clear(i, carry):
        wacc[:, pl.ds(pl.multiple_of(i * 512, 512), 512)] = jnp.zeros((width, 512), F32)
        return carry

    lax.fori_loop(0, model // 512, clear, 0)

    for copy in own_copies:
        copy.wait()
    for i, ref in arrays:
        for d in range(1, n):
            qkv_arrival(i, ref, d).wait_recv()

    kg = kg_ref[...]
    qg = qg_ref[...]
    for h in range(heads):
        cols = pl.ds(h * HEAD_DIM, HEAD_DIM)

        def prepare(j, carry, cols=cols):
            rows = pl.ds(pl.multiple_of(j * 256, 256), 256)
            keys = qkv[1, rows, cols].astype(F32)
            inverse = lax.rsqrt(jnp.mean(keys * keys, axis=-1, keepdims=True) + EPS)
            normed = keys * inverse * kg
            kn[rows, cols] = normed.astype(BF16)
            knt[cols, rows] = jnp.transpose(normed).astype(BF16)
            vt[cols, rows] = jnp.transpose(qkv[2, rows, cols].astype(F32)).astype(BF16)
            return carry

        lax.fori_loop(0, total // 256, prepare, 0)

    seg_k = seg_of(lax.broadcasted_iota(jnp.int32, (1, total), 1), ends_ref)
    do_copy.wait()
    w_copy.wait()

    def dq_copy(t):
        return pltpu.make_async_remote_copy(
            src_ref=dqs.at[t],
            dst_ref=dq_out.at[:, columns(me)],
            send_sem=dq_send.at[t],
            recv_sem=dq_recv.at[me],
            device_id={"seq": t},
            device_id_type=MESH,
        )

    def body(i, carry):
        step = (i + 1) // 2
        odd = lax.rem(i, 2)
        shift = sign * step
        t = lax.rem(me + shift - 2 * odd * shift + n, n)
        a_block = lax.rem(me - shift + n, n)
        b_block = lax.rem(me + shift + n, n)

        @pl.when(odd == 1)
        def _():
            for sub in range(SUBS):
                ring(0, step - 1, sub, a_block, up).wait_recv()

                @pl.when(step < a_steps)
                def _():
                    ring(0, step, sub, a_block, up).start()

            @pl.when(step <= b_steps)
            def _():
                for sub in range(SUBS):
                    ring(1, step - 1, sub, b_block, down).wait_recv()

                    @pl.when(step < b_steps)
                    def _():
                        ring(1, step, sub, b_block, down).start()

        datt[...] = jnp.zeros(datt.shape, F32)

        def project(j, c):
            part = pl.ds(pl.multiple_of(j * 1024, 1024), 1024)
            datt[...] += dot(do_all[t, :, part], w[:, part], NT)
            return c

        lax.fori_loop(0, model // 1024, project, 0)
        rows = rows_of(t)
        places = lax.broadcasted_iota(jnp.int32, (tokens, 1), 0) + t * tokens
        same = seg_of(places, ends_ref) == seg_k
        gain = jnp.zeros((1, HEAD_DIM), F32)
        for h in range(heads):
            cols = pl.ds(h * HEAD_DIM, HEAD_DIM)
            query = qkv[0, rows, cols].astype(F32)
            inverse = lax.rsqrt(jnp.mean(query * query, axis=-1, keepdims=True) + EPS)
            unit = query * inverse
            normed = unit * qg
            qn = normed.astype(BF16)
            expo = jnp.where(same, jnp.exp(dot(qn, knt[cols, :]) * scale), 0.0)
            probs = (expo * (1.0 / jnp.sum(expo, axis=-1, keepdims=True))).astype(BF16)
            attn = dot(probs, qkv[2, :, cols])
            attnt[cols, :] = jnp.transpose(attn).astype(BF16)
            dattn = datt[:, cols]
            d_probs = dot(dattn.astype(BF16), vt[cols, :])
            probs32 = probs.astype(F32)
            row_sum = jnp.sum(probs32 * d_probs, axis=-1, keepdims=True)
            d_scores = (probs32 * (d_probs - row_sum) * scale).astype(BF16)
            dvt[cols, :] += dot(jnp.transpose(dattn).astype(BF16), probs)
            dkt[cols, :] += dot(jnp.transpose(normed).astype(BF16), d_scores)
            d_normed = dot(d_scores, kn[:, cols])
            gain = gain + jnp.sum(unit * d_normed, axis=0, keepdims=True)
            d_unit = d_normed * qg
            d_query = inverse * (d_unit - unit * jnp.mean(unit * d_unit, axis=-1, keepdims=True))
            dqs[t, :, cols] = d_query.astype(BF16)
        gain_out[0:1, :] += gain

        @pl.when(i > 0)
        def _():
            dq_copy(t).start()

        def weigh(j, c):
            part = pl.ds(pl.multiple_of(j * 512, 512), 512)
            wacc[:, part] += dot(attnt[...], do_all[t, :, part])
            return c

        lax.fori_loop(0, model // 512, weigh, 0)
        return carry

    lax.fori_loop(0, n, body, 0)

    own_dq = pltpu.make_async_copy(dqs.at[me], dq_out.at[:, columns(me)], own_sem.at[0])
    own_dq.start()

    for h in range(heads):
        cols = pl.ds(h * HEAD_DIM, HEAD_DIM)

        def finish(j, gain, cols=cols):
            rows = pl.ds(pl.multiple_of(j * 256, 256), 256)
            keys = qkv[1, rows, cols].astype(F32)
            inverse = lax.rsqrt(jnp.mean(keys * keys, axis=-1, keepdims=True) + EPS)
            unit = keys * inverse
            d_normed = jnp.transpose(dkt[cols, rows])
            d_unit = d_normed * kg
            d_key = inverse * (d_unit - unit * jnp.mean(unit * d_unit, axis=-1, keepdims=True))
            dk_out[rows, cols] = d_key.astype(BF16)
            dv_out[rows, cols] = jnp.transpose(dvt[cols, rows]).astype(BF16)
            return gain + jnp.sum(unit * d_normed, axis=0, keepdims=True)

        gain = lax.fori_loop(0, total // 256, finish, jnp.zeros((1, HEAD_DIM), F32))
        gain_out[1:2, :] += gain

    def narrow(i, carry):
        part = pl.ds(pl.multiple_of(i * 512, 512), 512)
        wp_out[:, part] = wacc[:, part].astype(BF16)
        return carry

    lax.fori_loop(0, model // 512, narrow, 0)

    own_dq.wait()
    for i, ref in arrays:
        for d in order:
            qkv_copy(i, ref, d).wait_send()
    for sub in range(SUBS):
        for step in range(a_steps):
            ring(0, step, sub, me, up).wait_send()
        for step in range(b_steps):
            ring(1, step, sub, me, down).wait_send()
    for d in range(1, n):
        dq_copy(peer(d)).wait_send()
        source = peer(d)
        pltpu.make_async_remote_copy(
            src_ref=dqs.at[source],
            dst_ref=dq_out.at[:, columns(source)],
            send_sem=dq_send.at[source],
            recv_sem=dq_recv.at[source],
            device_id={"seq": source},
            device_id_type=MESH,
        ).wait_recv()


def exchange_kernel(
    n,
    side,
    dk_ref,
    dv_ref,
    wp_ref,
    dk_out,
    dv_out,
    sum_out,
    mine,
    theirs,
    packed,
    slots,
    reduced,
    final,
    z_send,
    z_recv,
    c_send,
    c_recv,
    x_send,
    x_recv,
    own_sem,
):
    me = lax.axis_index("seq")
    y, x, core = (lax.axis_index(name) for name in DP)
    other = 1 - core
    tokens = dk_out.shape[0]
    width = dk_ref.shape[1]
    rows_half = wp_ref.shape[0] // 2
    chips = side * side
    chunk = wp_ref.shape[1] // chips
    here = y * side + x

    def peer(d):
        return lax.rem(me + d, n)

    def columns(index):
        return pl.ds(pl.multiple_of(index * width, width), width)

    def rows_of(index):
        return pl.ds(pl.multiple_of(index * tokens, tokens), tokens)

    def chunk_of(index):
        return pl.ds(pl.multiple_of(index * chunk, chunk), chunk)

    def chip(d):
        place = lax.rem(here + d, chips)
        return {"dp_0": place // side, "dp_1": lax.rem(place, side)}, place

    barrier = pltpu.get_barrier_semaphore()
    for d in range(1, n):
        pl.semaphore_signal(barrier, inc=1, device_id={"seq": peer(d)}, device_id_type=MESH)
    for d in range(1, chips):
        pl.semaphore_signal(barrier, inc=1, device_id=chip(d)[0], device_id_type=MESH)
    pl.semaphore_signal(barrier, inc=1, device_id={"dp_2": other}, device_id_type=MESH)
    half_of = lambda c: pl.ds(pl.multiple_of(c * rows_half, rows_half), rows_half)
    mine_copy = pltpu.make_async_copy(wp_ref.at[half_of(core)], mine, own_sem.at[0])
    own = [
        pltpu.make_async_copy(ref.at[rows_of(me)], out.at[:, columns(me)], own_sem.at[1 + i])
        for i, (ref, out) in enumerate(((dk_ref, dk_out), (dv_ref, dv_out)))
    ]
    for copy in [mine_copy] + own:
        copy.start()
    pl.semaphore_wait(barrier, n + chips - 1)

    swap = pltpu.make_async_remote_copy(
        src_ref=wp_ref.at[half_of(other)],
        dst_ref=theirs,
        send_sem=c_send.at[0],
        recv_sem=c_recv.at[0],
        device_id={"dp_2": other},
        device_id_type=MESH,
    )
    swap.start()

    def back(i, ref, out, d, place):
        to = peer(d)
        return pltpu.make_async_remote_copy(
            src_ref=ref.at[rows_of(to)],
            dst_ref=out.at[:, columns(place)],
            send_sem=z_send.at[i, d],
            recv_sem=z_recv.at[i, place],
            device_id={"seq": to},
            device_id_type=MESH,
        )

    order = [4, 3, 5, 2, 6, 1, 7] if n == 8 else list(range(1, n))
    for i, (ref, out) in enumerate(((dk_ref, dk_out), (dv_ref, dv_out))):
        for d in order:
            back(i, ref, out, d, me).start()

    mine_copy.wait()
    swap.wait_recv()

    def merge(i, carry):
        part = chunk_of(i)
        packed[i] = (mine[:, part].astype(F32) + theirs[:, part].astype(F32)).astype(BF16)
        return carry

    lax.fori_loop(0, chips, merge, 0)

    def scatter(d, place_here):
        target, place = chip(d)
        return pltpu.make_async_remote_copy(
            src_ref=packed.at[place],
            dst_ref=slots.at[place_here],
            send_sem=x_send.at[d],
            recv_sem=x_recv.at[place_here],
            device_id=target,
            device_id_type=MESH,
        )

    for d in range(1, chips):
        scatter(d, here).start()
    reduced[...] = packed[here].astype(F32)
    for d in range(1, chips):
        place = chip(d)[1]
        scatter(d, place).wait_recv()
        reduced[...] += slots[place].astype(F32)

    window = pl.ds(pl.multiple_of(other * 128, 128), 256)
    last = pltpu.make_async_remote_copy(
        src_ref=reduced.at[:, window],
        dst_ref=final,
        send_sem=c_send.at[1],
        recv_sem=c_recv.at[1],
        device_id={"dp_2": other},
        device_id_type=MESH,
    )
    last.start()

    def pick(block):
        return jnp.where(core == 0, block[:, :192], block[:, 64:256])

    sum_out[half_of(core), :] = pick(reduced[:, pl.ds(pl.multiple_of(core * 128, 128), 256)])
    last.wait_recv()
    sum_out[half_of(other), :] = pick(final[...])
    last.wait_send()
    swap.wait_send()
    for d in range(1, chips):
        scatter(d, here).wait_send()
    for copy in own:
        copy.wait()
    for i, (ref, out) in enumerate(((dk_ref, dk_out), (dv_ref, dv_out))):
        for d in range(1, n):
            back(i, ref, out, d, me).wait_send()
            back(i, ref, out, d, peer(d)).wait_recv()


def norm_kernel(
    n,
    side,
    shard_ref,
    gain_ref,
    w_out,
    gain_out,
    norm_out,
    z_slots,
    dp_slots,
    z_send,
    z_recv,
    dp_send,
    dp_recv,
):
    me = lax.axis_index("seq")
    y, x, core = (lax.axis_index(name) for name in DP)
    group = 2 * side * side
    here = (y * side + x) * 2 + core

    def z_peer(d):
        return {"seq": lax.rem(me + d, n)}, lax.rem(me + d, n)

    def dp_peer(d):
        place = lax.rem(here + d, group)
        return {
            "dp_0": place // (2 * side),
            "dp_1": lax.rem(place // 2, side),
            "dp_2": lax.rem(place, 2),
        }, place

    barrier = pltpu.get_barrier_semaphore()
    for d in range(1, n):
        pl.semaphore_signal(barrier, inc=1, device_id=z_peer(d)[0], device_id_type=MESH)
    for d in range(1, group):
        pl.semaphore_signal(barrier, inc=1, device_id=dp_peer(d)[0], device_id_type=MESH)

    shard = shard_ref[...]
    square = jnp.sum(shard * shard)
    row = lax.broadcasted_iota(jnp.int32, (8, 128), 0)
    z_slots[me] = jnp.where(row == 2, square, gain_ref[...])
    pl.semaphore_wait(barrier, n + group - 2)

    def spread(slots, peer, count, sends, recvs, place):
        def send(d):
            return pltpu.make_async_remote_copy(
                src_ref=slots.at[place],
                dst_ref=slots.at[place],
                send_sem=sends.at[d],
                recv_sem=recvs.at[place],
                device_id=peer(d)[0],
                device_id_type=MESH,
            )

        def arrive(d):
            target, source = peer(d)
            return pltpu.make_async_remote_copy(
                src_ref=slots.at[source],
                dst_ref=slots.at[source],
                send_sem=sends.at[d],
                recv_sem=recvs.at[source],
                device_id=target,
                device_id_type=MESH,
            )

        for d in range(1, count):
            send(d).start()
        for d in range(1, count):
            arrive(d).wait_recv()
        for d in range(1, count):
            send(d).wait_send()
        total = slots[0]
        for place in range(1, count):
            total = total + slots[place]
        return total

    dp_slots[here] = spread(z_slots, z_peer, n, z_send, z_recv, me)
    total = spread(dp_slots, dp_peer, group, dp_send, dp_recv, here)
    gains = jnp.where(row < 2, total, 0.0)
    squares = jnp.sum(total[2:3, 0:1]) + jnp.sum(gains * gains)
    norm = jnp.sqrt(jnp.full((8, 128), squares, F32))
    factor = jnp.minimum(1.0, MAX_NORM / (norm + EPS))
    gain_out[...] = gains * factor
    norm_out[...] = norm
    w_out[...] = shard * factor[0:1, 0:1]


def local(n, side, query_rows, key_rows, value_rows, out_grad, clip_lengths, out_weight, query_gain, key_gain):
    tokens, inner = query_rows.shape[1:]
    model = out_grad.shape[2]
    width = inner // n
    total = tokens * n
    ends = jnp.cumsum(clip_lengths[0])
    vmem = pl.BlockSpec(memory_space=pltpu.VMEM)
    smem = pl.BlockSpec(memory_space=pltpu.SMEM)
    anywhere = pl.BlockSpec(memory_space=pl.ANY)
    dma = pltpu.SemaphoreType.DMA
    struct = jax.ShapeDtypeStruct
    chips = side * side
    dq, dk, dv, wp, gain = pl.pallas_call(
        functools.partial(attention_kernel, n),
        out_shape=(
            struct((tokens, inner), BF16),
            struct((total, width), BF16),
            struct((total, width), BF16),
            struct((width, model), BF16),
            struct((8, HEAD_DIM), F32),
        ),
        in_specs=[anywhere] * 5 + [smem, vmem, vmem],
        out_specs=(anywhere, vmem, vmem, vmem, vmem),
        scratch_shapes=[
            pltpu.VMEM((3, total, width), BF16),
            pltpu.VMEM((total, width), BF16),
            pltpu.VMEM((width, total), BF16),
            pltpu.VMEM((width, total), BF16),
            pltpu.VMEM((n, tokens, model), BF16),
            pltpu.VMEM((width, model), BF16),
            pltpu.VMEM((width, model), F32),
            pltpu.VMEM((width, total), F32),
            pltpu.VMEM((width, total), F32),
            pltpu.VMEM((tokens, width), F32),
            pltpu.VMEM((width, tokens), BF16),
            pltpu.VMEM((n, tokens, width), BF16),
            dma((3, n)),
            dma((3, n)),
            dma((2, n // 2, SUBS)),
            dma((n, SUBS)),
            dma((n,)),
            dma((n,)),
            dma((5,)),
        ],
        compiler_params=pltpu.CompilerParams(
            collective_id=1, has_side_effects=True, vmem_limit_bytes=60 * 1024 * 1024
        ),
        name="attention",
    )(
        query_rows[0],
        key_rows[0],
        value_rows[0],
        out_grad[0],
        out_weight,
        ends,
        query_gain[None],
        key_gain[None],
    )
    dk_back, dv_back, shard = pl.pallas_call(
        functools.partial(exchange_kernel, n, side),
        out_shape=(
            struct((tokens, inner), BF16),
            struct((tokens, inner), BF16),
            struct((width, model // (2 * chips)), F32),
        ),
        in_specs=[anywhere] * 3,
        out_specs=(anywhere, anywhere, vmem),
        scratch_shapes=[
            pltpu.VMEM((width // 2, model), BF16),
            pltpu.VMEM((width // 2, model), BF16),
            pltpu.VMEM((chips, width // 2, model // chips), BF16),
            pltpu.VMEM((chips, width // 2, model // chips), BF16),
            pltpu.VMEM((width // 2, model // chips), F32),
            pltpu.VMEM((width // 2, 256), F32),
            dma((2, n)),
            dma((2, n)),
            dma((2,)),
            dma((2,)),
            dma((chips,)),
            dma((chips,)),
            dma((3,)),
        ],
        compiler_params=pltpu.CompilerParams(
            collective_id=2, has_side_effects=True, vmem_limit_bytes=60 * 1024 * 1024
        ),
        name="exchange",
    )(dk, dv, wp)
    weight_grad, gains, norm = pl.pallas_call(
        functools.partial(norm_kernel, n, side),
        out_shape=(
            struct(shard.shape, F32),
            struct((8, HEAD_DIM), F32),
            struct((8, 128), F32),
        ),
        in_specs=[vmem, vmem],
        out_specs=(vmem, vmem, vmem),
        scratch_shapes=[
            pltpu.VMEM((n, 8, 128), F32),
            pltpu.VMEM((2 * chips, 8, 128), F32),
            dma((n,)),
            dma((n,)),
            dma((2 * chips,)),
            dma((2 * chips,)),
        ],
        compiler_params=pltpu.CompilerParams(collective_id=3, has_side_effects=True),
        name="norm",
    )(shard, gain)
    return (
        dq[None],
        dk_back[None],
        dv_back[None],
        weight_grad,
        gains[0],
        gains[1],
        norm[0, 0],
    )


def solution(mesh):
    n = mesh.shape["seq"]
    torus = Mesh(mesh.devices.reshape(4, 4, 2, n), ("dp_0", "dp_1", "dp_2", "seq"))
    return jax.shard_map(
        functools.partial(local, n, 4),
        mesh=torus,
        in_specs=(
            P(DP, "seq", None),
            P(DP, "seq", None),
            P(DP, "seq", None),
            P(DP, "seq", None),
            P(DP, None),
            P("seq", None),
            P(),
            P(),
        ),
        out_specs=(
            P(DP, "seq", None),
            P(DP, "seq", None),
            P(DP, "seq", None),
            P("seq", DP),
            P(),
            P(),
            P(),
        ),
        check_vma=False,
    )
```

```python
import functools

import jax
import jax.numpy as jnp
from jax import lax
from jax.experimental import pallas as pl
from jax.experimental.pallas import tpu as pltpu
from jax.sharding import Mesh
from jax.sharding import PartitionSpec as P

HEAD_DIM = 128
MAX_NORM = 768
EPS = 1e-06
DP = ("dp_0", "dp_1", "dp_2")
MESH = pl.DeviceIdType.MESH
F32 = jnp.float32
BF16 = jnp.bfloat16
NN = (((1,), (0,)), ((), ()))
NT = (((1,), (1,)), ((), ()))
SUBS = 4


def dot(a, b, dims=NN):
    return lax.dot_general(a, b, dims, preferred_element_type=F32)


def seg_of(places, lengths_ref):
    seg = jnp.zeros(places.shape, jnp.int32)
    end = jnp.int32(0)
    for c in range(lengths_ref.shape[0]):
        end = end + lengths_ref[c]
        seg = seg + (places >= end).astype(jnp.int32)
    return seg


def kernel(
    n,
    side,
    q_hbm,
    k_hbm,
    v_hbm,
    do_hbm,
    w_hbm,
    lengths_ref,
    qg_ref,
    kg_ref,
    dq_out,
    dk_out,
    dv_out,
    w_out,
    qgain_out,
    kgain_out,
    norm_out,
    qkv,
    kn,
    knt,
    vt,
    do_all,
    w,
    wacc,
    dkt,
    dvt,
    datt,
    attnt,
    probs,
    dqs,
    dkv,
    gain,
    wpb,
    theirs,
    packed,
    slots,
    reduced,
    final,
    z_slots,
    dp_slots,
    qkv_send,
    qkv_recv,
    ag_send,
    ag_recv,
    dq_send,
    dq_recv,
    dkv_send,
    dkv_recv,
    swap_send,
    swap_recv,
    x_send,
    x_recv,
    last_send,
    last_recv,
    z_send,
    z_recv,
    dp_send,
    dp_recv,
    own_sem,
):
    me = lax.axis_index("seq")
    y, x, core = (lax.axis_index(name) for name in DP)
    other = 1 - core
    sign = 1 - 2 * core
    tokens = q_hbm.shape[0]
    total = tokens * n
    width = q_hbm.shape[1] // n
    heads = width // HEAD_DIM
    model = do_hbm.shape[1]
    quarter = model // SUBS
    scale = HEAD_DIM ** (-0.5)
    up = lax.rem(me + sign + n, n)
    down = lax.rem(me - sign + n, n)
    a_steps = n // 2
    b_steps = n - 1 - a_steps
    chips = side * side
    chunk = model // chips
    per_sub = chips // SUBS
    half = width // 2
    here = y * side + x
    group = 2 * chips
    in_group = here * 2 + core

    def columns(index):
        return pl.ds(pl.multiple_of(index * width, width), width)

    def rows_of(index):
        return pl.ds(pl.multiple_of(index * tokens, tokens), tokens)

    def half_of(index):
        return pl.ds(pl.multiple_of(index * half, half), half)

    def sub_of(index):
        return pl.ds(index * quarter, quarter)

    def peer(d):
        return lax.rem(me + d, n)

    def z_peer(d):
        return {"seq": peer(d)}, peer(d)

    def chip(d):
        place = lax.rem(here + d, chips)
        return {"dp_0": place // side, "dp_1": lax.rem(place, side)}, place

    def dp_peer(d):
        place = lax.rem(in_group + d, group)
        return {
            "dp_0": place // (2 * side),
            "dp_1": lax.rem(place // 2, side),
            "dp_2": lax.rem(place, 2),
        }, place

    def remote(src, dst, send, recv, to):
        return pltpu.make_async_remote_copy(
            src_ref=src, dst_ref=dst, send_sem=send, recv_sem=recv, device_id=to, device_id_type=MESH
        )

    barrier = pltpu.get_barrier_semaphore()
    for d in range(1, n):
        pl.semaphore_signal(barrier, inc=1, device_id=z_peer(d)[0], device_id_type=MESH)
    for d in range(1, group):
        pl.semaphore_signal(barrier, inc=1, device_id=dp_peer(d)[0], device_id_type=MESH)

    own_copies = [
        pltpu.make_async_copy(ref.at[:, columns(me)], qkv.at[i, rows_of(me)], own_sem.at[i])
        for i, ref in enumerate((q_hbm, k_hbm, v_hbm))
    ]
    do_copies = [
        pltpu.make_async_copy(do_hbm.at[:, sub_of(sub)], do_all.at[me, sub], own_sem.at[4 + sub])
        for sub in range(SUBS)
    ]
    w_copy = pltpu.make_async_copy(w_hbm, w, own_sem.at[3])
    for copy in own_copies + do_copies + [w_copy]:
        copy.start()
    pl.semaphore_wait(barrier, n + group - 2)

    order = [4, 3, 5, 2, 6, 1, 7] if n == 8 else list(range(1, n))
    arrays = ((1, k_hbm), (2, v_hbm), (0, q_hbm))

    def qkv_copy(i, ref, d, place):
        to = peer(d)
        return remote(
            ref.at[:, columns(to)],
            qkv.at[i, rows_of(place)],
            qkv_send.at[i, d],
            qkv_recv.at[i, place],
            {"seq": to},
        )

    for i, ref in arrays:
        for d in order:
            qkv_copy(i, ref, d, me).start()

    def ring(direction, step, sub, block, to, own=False):
        return remote(
            do_hbm.at[:, sub_of(sub)] if own else do_all.at[block, sub],
            do_all.at[block, sub],
            ag_send.at[direction, step, sub],
            ag_recv.at[block, sub],
            {"seq": to},
        )

    for sub in range(SUBS):
        ring(0, 0, sub, me, up, True).start()
        ring(1, 0, sub, me, down, True).start()

    dkt[...] = jnp.zeros(dkt.shape, F32)
    dvt[...] = jnp.zeros(dvt.shape, F32)
    gain[...] = jnp.zeros(gain.shape, F32)

    def clear(i, carry):
        wacc[:, pl.ds(pl.multiple_of(i * 512, 512), 512)] = jnp.zeros((width, 512), F32)
        return carry

    lax.fori_loop(0, model // 512, clear, 0)
    kg = kg_ref[...]
    qg = qg_ref[...]
    seg_k = seg_of(lax.broadcasted_iota(jnp.int32, (1, total), 1), lengths_ref)

    for copy in own_copies:
        copy.wait()
    for i, ref in arrays:
        for d in range(1, n):
            qkv_copy(i, ref, d, peer(d)).wait_recv()

    def norm_rows(i, rows, cols):
        block = qkv[i, rows, cols].astype(F32)
        inverse = lax.rsqrt(jnp.mean(block * block, axis=-1, keepdims=True) + EPS)
        return block * inverse, inverse

    def norm_back(unit, inverse, weight, d_normed):
        d_unit = d_normed * weight
        d_rows = inverse * (d_unit - unit * jnp.mean(unit * d_unit, axis=-1, keepdims=True))
        return d_rows.astype(BF16)

    for h in range(heads):
        cols = pl.ds(h * HEAD_DIM, HEAD_DIM)

        def prepare(j, carry, cols=cols):
            rows = pl.ds(pl.multiple_of(j * 256, 256), 256)
            normed = norm_rows(1, rows, cols)[0] * kg
            kn[rows, cols] = normed.astype(BF16)
            knt[cols, rows] = jnp.transpose(normed).astype(BF16)
            vt[cols, rows] = jnp.transpose(qkv[2, rows, cols].astype(F32)).astype(BF16)
            return carry

        lax.fori_loop(0, total // 256, prepare, 0)

    def forward(j, carry):
        rows = pl.ds(pl.multiple_of(j * 256, 256), 256)
        places = lax.broadcasted_iota(jnp.int32, (256, 1), 0) + j * 256
        same = seg_of(places, lengths_ref) == seg_k
        for h in range(heads):
            cols = pl.ds(h * HEAD_DIM, HEAD_DIM)
            qn = (norm_rows(0, rows, cols)[0] * qg).astype(BF16)
            expo = jnp.where(same, jnp.exp(dot(qn, knt[cols, :]) * scale), 0.0)
            prob = (expo * (1.0 / jnp.sum(expo, axis=-1, keepdims=True))).astype(BF16)
            probs[h, rows, :] = prob
            attn = dot(prob, qkv[2, :, cols])
            attnt[cols, rows] = jnp.transpose(attn).astype(BF16)
        return carry

    lax.fori_loop(0, total // 256, forward, 0)
    for copy in do_copies:
        copy.wait()
    w_copy.wait()

    def project(t, sub):
        part = sub_of(sub)
        datt[...] += dot(do_all[t, sub], w[:, part], NT)

    def weigh(t, sub):
        def piece(j, c):
            part = pl.ds(pl.multiple_of(j * 512, 512), 512)
            into = pl.ds(pl.multiple_of(sub * quarter + j * 512, 512), 512)
            wacc[:, into] += dot(attnt[:, rows_of(t)], do_all[t, sub, :, part])
            return c

        lax.fori_loop(0, quarter // 512, piece, 0)

    def backward(t, h):
        rows = rows_of(t)
        cols = pl.ds(h * HEAD_DIM, HEAD_DIM)
        unit, inverse = norm_rows(0, rows, cols)
        normed = unit * qg
        dattn = datt[:, cols]
        prob = probs[h, rows, :]
        prob32 = prob.astype(F32)
        d_probs = dot(dattn.astype(BF16), vt[cols, :])
        row_sum = jnp.sum(prob32 * d_probs, axis=-1, keepdims=True)
        d_scores = (prob32 * (d_probs - row_sum) * scale).astype(BF16)
        dvt[cols, :] += dot(jnp.transpose(dattn).astype(BF16), prob)
        dkt[cols, :] += dot(jnp.transpose(normed).astype(BF16), d_scores)
        d_normed = dot(d_scores, kn[:, cols])
        gain[0:1, :] += jnp.sum(unit * d_normed, axis=0, keepdims=True)
        dqs[t, :, cols] = norm_back(unit, inverse, qg, d_normed)

    def dq_copy(t, place):
        return remote(
            dqs.at[t], dq_out.at[:, columns(place)], dq_send.at[t], dq_recv.at[place], {"seq": t}
        )

    def body(i, carry):
        step = (i + 1) // 2
        odd = lax.rem(i, 2)
        shift = sign * step
        t = lax.rem(me + shift - 2 * odd * shift + n, n)
        a_block = lax.rem(me - shift + n, n)
        b_block = lax.rem(me + shift + n, n)

        @pl.when(odd == 1)
        def _():
            for sub in range(SUBS):
                ring(0, step - 1, sub, a_block, up).wait_recv()
                ring(0, step, sub, a_block, up).start()
            for sub in range(SUBS):
                ring(1, step - 1, sub, b_block, down).wait_recv()

                @pl.when(step < b_steps)
                def _():
                    ring(1, step, sub, b_block, down).start()

        datt[...] = jnp.zeros(datt.shape, F32)
        for sub in range(SUBS):
            project(t, sub)
        for h in range(heads):
            backward(t, h)

        @pl.when(i > 0)
        def _():
            dq_copy(t, me).start()

        for sub in range(SUBS):
            weigh(t, sub)
        return carry

    lax.fori_loop(0, n - 1, body, 0)

    own_dq = pltpu.make_async_copy(dqs.at[me], dq_out.at[:, columns(me)], own_sem.at[0])
    own_dq.start()

    t = lax.rem(me - sign * a_steps + n, n)
    datt[...] = jnp.zeros(datt.shape, F32)

    def swap(sub):
        part = sub_of(sub)
        return remote(
            wpb.at[half_of(other), part],
            theirs.at[:, part],
            swap_send.at[sub],
            swap_recv.at[sub],
            {"dp_2": other},
        )

    def scatter(d, place_here):
        target, place = chip(d)
        return remote(
            packed.at[place], slots.at[place_here], x_send.at[place], x_recv.at[place_here], target
        )

    def merge(sub):
        swap(sub).wait_recv()

        def piece(j, carry):
            part = pl.ds(pl.multiple_of(j * chunk, chunk), chunk)
            packed[j] = (wpb[half_of(core), part].astype(F32) + theirs[:, part].astype(F32)).astype(BF16)
            return carry

        lax.fori_loop(sub * per_sub, (sub + 1) * per_sub, piece, 0)

    def scatter_of(place):
        return remote(
            packed.at[place],
            slots.at[here],
            x_send.at[place],
            x_recv.at[here],
            {"dp_0": place // side, "dp_1": lax.rem(place, side)},
        )

    def send_sub(sub):
        def one(j, carry):
            place = sub * per_sub + lax.rem(here + j, per_sub)

            @pl.when(place != here)
            def _():
                scatter_of(place).start()

            return carry

        lax.fori_loop(0, per_sub, one, 0)

    for sub in range(SUBS):
        ring(0, a_steps - 1, sub, t, up).wait_recv()
        weigh(t, sub)

        def narrow(j, carry, sub=sub):
            part = pl.ds(pl.multiple_of(sub * quarter + j * 512, 512), 512)
            wpb[:, part] = wacc[:, part].astype(BF16)
            return carry

        lax.fori_loop(0, quarter // 512, narrow, 0)
        if sub > 0:
            merge(sub - 1)
        project(t, sub)
        swap(sub).start()
        if sub > 0:
            send_sub(sub - 1)

    def dkv_copy(i, h, d, place):
        to = peer(d)
        return remote(
            dkv.at[i, rows_of(to), pl.ds(h * HEAD_DIM, HEAD_DIM)],
            (dk_out, dv_out)[i].at[:, pl.ds(pl.multiple_of(place * width + h * HEAD_DIM, HEAD_DIM), HEAD_DIM)],
            dkv_send.at[i, h, d],
            dkv_recv.at[i, h, place],
            {"seq": to},
        )

    for h in range(heads):
        cols = pl.ds(h * HEAD_DIM, HEAD_DIM)
        backward(t, h)

        def finish(j, carry, cols=cols):
            rows = pl.ds(pl.multiple_of(j * 256, 256), 256)
            dkv[1, rows, cols] = jnp.transpose(dvt[cols, rows]).astype(BF16)
            unit, inverse = norm_rows(1, rows, cols)
            d_normed = jnp.transpose(dkt[cols, rows])
            gain[1:2, :] += jnp.sum(unit * d_normed, axis=0, keepdims=True)
            dkv[0, rows, cols] = norm_back(unit, inverse, kg, d_normed)
            return carry

        lax.fori_loop(0, total // 256, finish, 0)
        for i in (1, 0):
            for d in order:
                dkv_copy(i, h, d, me).start()
        if h == 0:
            merge(SUBS - 1)
            send_sub(SUBS - 1)
    dq_copy(t, me).start()
    own_dkv = [
        pltpu.make_async_copy(dkv.at[i, rows_of(me)], out.at[:, columns(me)], own_sem.at[1 + i])
        for i, out in enumerate((dk_out, dv_out))
    ]
    for copy in own_dkv:
        copy.start()

    reduced[...] = packed[here].astype(F32)
    for d in range(1, chips):
        place = chip(d)[1]
        scatter(d, place).wait_recv()
        reduced[...] += slots[place].astype(F32)

    def window(index):
        return pl.ds(pl.multiple_of(index * 128, 128), 256)

    shard_width = chunk // 2
    last = remote(reduced.at[:, window(other)], final, last_send.at[0], last_recv.at[0], {"dp_2": other})
    last.start()

    def pick(block):
        return jnp.where(core == 0, block[:, :shard_width], block[:, 256 - shard_width :])

    mine = pick(reduced[:, window(core)])
    w_out[half_of(core), :] = mine
    square = jnp.sum(mine * mine)
    row = lax.broadcasted_iota(jnp.int32, (8, 128), 0)
    last.wait_recv()
    rest = pick(final[...])
    w_out[half_of(other), :] = rest
    square = square + jnp.sum(rest * rest)
    z_slots[me] = jnp.where(row == 2, square, gain[...])

    def spread(buffer, peers, count, sends, recvs, place):
        def copy(d, source):
            return remote(buffer.at[source], buffer.at[source], sends.at[d], recvs.at[source], peers(d)[0])

        for d in range(1, count):
            copy(d, place).start()
        for d in range(1, count):
            copy(d, peers(d)[1]).wait_recv()
        result = buffer[0]
        for index in range(1, count):
            result = result + buffer[index]
        for d in range(1, count):
            copy(d, place).wait_send()
        return result

    dp_slots[in_group] = spread(z_slots, z_peer, n, z_send, z_recv, me)
    summed = spread(dp_slots, dp_peer, group, dp_send, dp_recv, in_group)
    gains = jnp.where(row < 2, summed, 0.0)
    squares = summed[2:3, 0:1] + jnp.sum(gains * gains)
    norm = jnp.sqrt(squares)
    factor = jnp.minimum(1.0, MAX_NORM / (norm + EPS))
    qgain_out[...] = gains[0:1] * factor
    kgain_out[...] = gains[1:2] * factor
    norm_out[...] = norm
    w_out[...] = w_out[...] * factor

    last.wait_send()
    own_dq.wait()
    for copy in own_dkv:
        copy.wait()
    for i, ref in arrays:
        for d in order:
            qkv_copy(i, ref, d, me).wait_send()
    for sub in range(SUBS):
        swap(sub).wait_send()
        for step in range(a_steps):
            ring(0, step, sub, me, up).wait_send()
        for step in range(b_steps):
            ring(1, step, sub, me, down).wait_send()
    for d in range(1, chips):
        scatter(d, here).wait_send()
    for d in range(1, n):
        dq_copy(peer(d), me).wait_send()
        dq_copy(peer(d), peer(d)).wait_recv()
        for i in (0, 1):
            for h in range(heads):
                dkv_copy(i, h, d, me).wait_send()
                dkv_copy(i, h, d, peer(d)).wait_recv()


def local(n, side, query_rows, key_rows, value_rows, out_grad, clip_lengths, out_weight, query_gain, key_gain):
    tokens, inner = query_rows.shape[1:]
    model = out_grad.shape[2]
    width = inner // n
    heads = width // HEAD_DIM
    total = tokens * n
    vmem = pl.BlockSpec(memory_space=pltpu.VMEM)
    smem = pl.BlockSpec(memory_space=pltpu.SMEM)
    anywhere = pl.BlockSpec(memory_space=pl.ANY)
    dma = pltpu.SemaphoreType.DMA
    struct = jax.ShapeDtypeStruct
    chips = side * side
    chunk = model // chips
    dq, dk, dv, weight_grad, qgain, kgain, norm = pl.pallas_call(
        functools.partial(kernel, n, side),
        out_shape=(
            struct((tokens, inner), BF16),
            struct((tokens, inner), BF16),
            struct((tokens, inner), BF16),
            struct((width, chunk // 2), F32),
            struct((1, HEAD_DIM), F32),
            struct((1, HEAD_DIM), F32),
            struct((1, 1), F32),
        ),
        in_specs=[anywhere] * 5 + [smem, vmem, vmem],
        out_specs=(anywhere, anywhere, anywhere, vmem, vmem, vmem, vmem),
        scratch_shapes=[
            pltpu.VMEM((3, total, width), BF16),
            pltpu.VMEM((total, width), BF16),
            pltpu.VMEM((width, total), BF16),
            pltpu.VMEM((width, total), BF16),
            pltpu.VMEM((n, SUBS, tokens, model // SUBS), BF16),
            pltpu.VMEM((width, model), BF16),
            pltpu.VMEM((width, model), F32),
            pltpu.VMEM((width, total), F32),
            pltpu.VMEM((width, total), F32),
            pltpu.VMEM((tokens, width), F32),
            pltpu.VMEM((width, total), BF16),
            pltpu.VMEM((heads, total, total), BF16),
            pltpu.VMEM((n, tokens, width), BF16),
            pltpu.VMEM((2, total, width), BF16),
            pltpu.VMEM((8, HEAD_DIM), F32),
            pltpu.VMEM((width, model), BF16),
            pltpu.VMEM((width // 2, model), BF16),
            pltpu.VMEM((chips, width // 2, chunk), BF16),
            pltpu.VMEM((chips, width // 2, chunk), BF16),
            pltpu.VMEM((width // 2, chunk), F32),
            pltpu.VMEM((width // 2, 256), F32),
            pltpu.VMEM((n, 8, 128), F32),
            pltpu.VMEM((2 * chips, 8, 128), F32),
            dma((3, n)),
            dma((3, n)),
            dma((2, n // 2, SUBS)),
            dma((n, SUBS)),
            dma((n,)),
            dma((n,)),
            dma((2, heads, n)),
            dma((2, heads, n)),
            dma((SUBS,)),
            dma((SUBS,)),
            dma((chips,)),
            dma((chips,)),
            dma((1,)),
            dma((1,)),
            dma((n,)),
            dma((n,)),
            dma((2 * chips,)),
            dma((2 * chips,)),
            dma((8,)),
        ],
        compiler_params=pltpu.CompilerParams(
            collective_id=1, has_side_effects=True, vmem_limit_bytes=67043328
        ),
        name="fused",
    )(
        query_rows[0],
        key_rows[0],
        value_rows[0],
        out_grad[0],
        out_weight,
        clip_lengths[0],
        query_gain[None],
        key_gain[None],
    )
    return (
        dq[None],
        dk[None],
        dv[None],
        weight_grad,
        qgain.reshape(HEAD_DIM),
        kgain.reshape(HEAD_DIM),
        norm.reshape(()),
    )


def solution(mesh):
    n = mesh.shape["seq"]
    torus = Mesh(mesh.devices.reshape(4, 4, 2, n), ("dp_0", "dp_1", "dp_2", "seq"))
    return jax.shard_map(
        functools.partial(local, n, 4),
        mesh=torus,
        in_specs=(
            P(DP, "seq", None),
            P(DP, "seq", None),
            P(DP, "seq", None),
            P(DP, "seq", None),
            P(DP, None),
            P("seq", None),
            P(),
            P(),
        ),
        out_specs=(
            P(DP, "seq", None),
            P(DP, "seq", None),
            P(DP, "seq", None),
            P("seq", DP),
            P(),
            P(),
            P(),
        ),
        check_vma=False,
    )
```

```python
import functools

import jax
import jax.numpy as jnp
from jax import lax
from jax.experimental import pallas as pl
from jax.experimental.pallas import tpu as pltpu
from jax.sharding import Mesh
from jax.sharding import PartitionSpec as P

HEAD_DIM = 128
MAX_NORM = 768
EPS = 1e-06
DP = ("dp_0", "dp_1", "dp_2")
MESH = pl.DeviceIdType.MESH
F32 = jnp.float32
BF16 = jnp.bfloat16
NN = (((1,), (0,)), ((), ()))
NT = (((1,), (1,)), ((), ()))
SUBS = 4


def dot(a, b, dims=NN):
    return lax.dot_general(a, b, dims, preferred_element_type=F32)


def seg_of(places, lengths_ref):
    seg = jnp.zeros(places.shape, jnp.int32)
    end = jnp.int32(0)
    for c in range(lengths_ref.shape[0]):
        end = end + lengths_ref[c]
        seg = seg + (places >= end).astype(jnp.int32)
    return seg


def kernel(
    n,
    side,
    q_hbm,
    k_hbm,
    v_hbm,
    do_hbm,
    w_hbm,
    lengths_ref,
    qg_ref,
    kg_ref,
    dq_out,
    dk_out,
    dv_out,
    w_out,
    qgain_out,
    kgain_out,
    norm_out,
    qkv,
    kn,
    knt,
    vt,
    do_all,
    w,
    wacc,
    dkt,
    dvt,
    datt,
    attnt,
    probs,
    dqs,
    dkv,
    gain,
    wpb,
    theirs,
    packed,
    slots,
    reduced,
    final,
    z_slots,
    dp_slots,
    qkv_send,
    qkv_recv,
    ag_send,
    ag_recv,
    dq_send,
    dq_recv,
    dkv_send,
    dkv_recv,
    swap_send,
    swap_recv,
    x_send,
    x_recv,
    last_send,
    last_recv,
    z_send,
    z_recv,
    dp_send,
    dp_recv,
    own_sem,
):
    me = lax.axis_index("seq")
    y, x, core = (lax.axis_index(name) for name in DP)
    other = 1 - core
    sign = 1 - 2 * core
    tokens = q_hbm.shape[0]
    total = tokens * n
    width = q_hbm.shape[1] // n
    heads = width // HEAD_DIM
    model = do_hbm.shape[1]
    quarter = model // SUBS
    scale = HEAD_DIM ** (-0.5)
    up = lax.rem(me + sign + n, n)
    down = lax.rem(me - sign + n, n)
    a_steps = n // 2
    b_steps = n - 1 - a_steps
    chips = side * side
    chunk = model // chips
    per_sub = chips // SUBS
    half = width // 2
    here = y * side + x
    group = 2 * chips
    in_group = here * 2 + core

    def columns(index):
        return pl.ds(pl.multiple_of(index * width, width), width)

    def rows_of(index):
        return pl.ds(pl.multiple_of(index * tokens, tokens), tokens)

    def half_of(index):
        return pl.ds(pl.multiple_of(index * half, half), half)

    def sub_of(index):
        return pl.ds(index * quarter, quarter)

    def peer(d):
        return lax.rem(me + d, n)

    def z_peer(d):
        return {"seq": peer(d)}, peer(d)

    def chip(d):
        place = lax.rem(here + d, chips)
        return {"dp_0": place // side, "dp_1": lax.rem(place, side)}, place

    def dp_peer(d):
        place = lax.rem(in_group + d, group)
        return {
            "dp_0": place // (2 * side),
            "dp_1": lax.rem(place // 2, side),
            "dp_2": lax.rem(place, 2),
        }, place

    def remote(src, dst, send, recv, to):
        return pltpu.make_async_remote_copy(
            src_ref=src, dst_ref=dst, send_sem=send, recv_sem=recv, device_id=to, device_id_type=MESH
        )

    barrier = pltpu.get_barrier_semaphore()
    for d in range(1, n):
        pl.semaphore_signal(barrier, inc=1, device_id=z_peer(d)[0], device_id_type=MESH)
    for d in range(1, group):
        pl.semaphore_signal(barrier, inc=1, device_id=dp_peer(d)[0], device_id_type=MESH)

    own_copies = [
        pltpu.make_async_copy(ref.at[:, columns(me)], qkv.at[i, rows_of(me)], own_sem.at[i])
        for i, ref in enumerate((q_hbm, k_hbm, v_hbm))
    ]
    do_copies = [
        pltpu.make_async_copy(do_hbm.at[:, sub_of(sub)], do_all.at[me, sub], own_sem.at[4 + sub])
        for sub in range(SUBS)
    ]
    w_copy = pltpu.make_async_copy(w_hbm, w, own_sem.at[3])
    for copy in own_copies + do_copies + [w_copy]:
        copy.start()
    pl.semaphore_wait(barrier, n + group - 2)

    order = [4, 3, 5, 2, 6, 1, 7] if n == 8 else list(range(1, n))
    arrays = ((1, k_hbm), (2, v_hbm), (0, q_hbm))

    def qkv_copy(i, ref, d, place):
        to = peer(d)
        return remote(
            ref.at[:, columns(to)],
            qkv.at[i, rows_of(place)],
            qkv_send.at[i, d],
            qkv_recv.at[i, place],
            {"seq": to},
        )

    for i, ref in arrays:
        for d in order:
            qkv_copy(i, ref, d, me).start()

    def ring(direction, step, sub, block, to, own=False):
        return remote(
            do_hbm.at[:, sub_of(sub)] if own else do_all.at[block, sub],
            do_all.at[block, sub],
            ag_send.at[direction, step, sub],
            ag_recv.at[block, sub],
            {"seq": to},
        )

    for sub in range(SUBS):
        ring(0, 0, sub, me, up, True).start()
        ring(1, 0, sub, me, down, True).start()

    dkt[...] = jnp.zeros(dkt.shape, F32)
    dvt[...] = jnp.zeros(dvt.shape, F32)
    gain[...] = jnp.zeros(gain.shape, F32)

    def clear(i, carry):
        wacc[:, pl.ds(pl.multiple_of(i * 512, 512), 512)] = jnp.zeros((width, 512), F32)
        return carry

    lax.fori_loop(0, model // 512, clear, 0)
    kg = kg_ref[...]
    qg = qg_ref[...]
    seg_k = seg_of(lax.broadcasted_iota(jnp.int32, (1, total), 1), lengths_ref)

    for copy in own_copies:
        copy.wait()
    for i, ref in arrays:
        for d in range(1, n):
            qkv_copy(i, ref, d, peer(d)).wait_recv()

    def norm_rows(i, rows, cols):
        block = qkv[i, rows, cols].astype(F32)
        inverse = lax.rsqrt(jnp.mean(block * block, axis=-1, keepdims=True) + EPS)
        return block * inverse, inverse

    def norm_back(unit, inverse, weight, d_normed):
        d_unit = d_normed * weight
        d_rows = inverse * (d_unit - unit * jnp.mean(unit * d_unit, axis=-1, keepdims=True))
        return d_rows.astype(BF16)

    for h in range(heads):
        cols = pl.ds(h * HEAD_DIM, HEAD_DIM)

        def prepare(j, carry, cols=cols):
            rows = pl.ds(pl.multiple_of(j * 256, 256), 256)
            normed = norm_rows(1, rows, cols)[0] * kg
            kn[rows, cols] = normed.astype(BF16)
            knt[cols, rows] = jnp.transpose(normed).astype(BF16)
            vt[cols, rows] = jnp.transpose(qkv[2, rows, cols].astype(F32)).astype(BF16)
            return carry

        lax.fori_loop(0, total // 256, prepare, 0)

    def forward(j, carry):
        rows = pl.ds(pl.multiple_of(j * 256, 256), 256)
        places = lax.broadcasted_iota(jnp.int32, (256, 1), 0) + j * 256
        same = seg_of(places, lengths_ref) == seg_k
        for h in range(heads):
            cols = pl.ds(h * HEAD_DIM, HEAD_DIM)
            qn = (norm_rows(0, rows, cols)[0] * qg).astype(BF16)
            expo = jnp.where(same, jnp.exp(dot(qn, knt[cols, :]) * scale), 0.0)
            prob = (expo * (1.0 / jnp.sum(expo, axis=-1, keepdims=True))).astype(BF16)
            probs[h, rows, :] = prob
            attn = dot(prob, qkv[2, :, cols])
            attnt[cols, rows] = jnp.transpose(attn).astype(BF16)
        return carry

    lax.fori_loop(0, total // 256, forward, 0)
    for copy in do_copies:
        copy.wait()
    w_copy.wait()

    def project(t, sub):
        part = sub_of(sub)
        datt[...] += dot(do_all[t, sub], w[:, part], NT)

    def weigh(t, sub):
        def piece(j, c):
            part = pl.ds(pl.multiple_of(j * 512, 512), 512)
            into = pl.ds(pl.multiple_of(sub * quarter + j * 512, 512), 512)
            wacc[:, into] += dot(attnt[:, rows_of(t)], do_all[t, sub, :, part])
            return c

        lax.fori_loop(0, quarter // 512, piece, 0)

    def backward(t, h):
        rows = rows_of(t)
        cols = pl.ds(h * HEAD_DIM, HEAD_DIM)
        unit, inverse = norm_rows(0, rows, cols)
        normed = unit * qg
        dattn = datt[:, cols]
        prob = probs[h, rows, :]
        prob32 = prob.astype(F32)
        d_probs = dot(dattn.astype(BF16), vt[cols, :])
        row_sum = jnp.sum(prob32 * d_probs, axis=-1, keepdims=True)
        d_scores = (prob32 * (d_probs - row_sum) * scale).astype(BF16)
        dvt[cols, :] += dot(jnp.transpose(dattn).astype(BF16), prob)
        dkt[cols, :] += dot(jnp.transpose(normed).astype(BF16), d_scores)
        d_normed = dot(d_scores, kn[:, cols])
        gain[0:1, :] += jnp.sum(unit * d_normed, axis=0, keepdims=True)
        dqs[t, :, cols] = norm_back(unit, inverse, qg, d_normed)

    def dq_copy(t, place):
        return remote(
            dqs.at[t], dq_out.at[:, columns(place)], dq_send.at[t], dq_recv.at[place], {"seq": t}
        )

    def body(i, carry):
        step = (i + 1) // 2
        odd = lax.rem(i, 2)
        shift = sign * step
        t = lax.rem(me + shift - 2 * odd * shift + n, n)
        a_block = lax.rem(me - shift + n, n)
        b_block = lax.rem(me + shift + n, n)

        @pl.when(odd == 1)
        def _():
            for sub in range(SUBS):
                ring(0, step - 1, sub, a_block, up).wait_recv()
                ring(0, step, sub, a_block, up).start()
                ring(1, step - 1, sub, b_block, down).wait_recv()

                @pl.when(step < b_steps)
                def _():
                    ring(1, step, sub, b_block, down).start()

        datt[...] = jnp.zeros(datt.shape, F32)
        for sub in range(SUBS):
            project(t, sub)
        for h in range(heads):
            backward(t, h)

        for sub in range(SUBS):
            weigh(t, sub)

        @pl.when(i == 2 * b_steps - 1)
        def _():
            def early(j, c):
                dq_copy(lax.rem(me + sign * (j - b_steps) + n, n), me).start()
                return c

            lax.fori_loop(0, b_steps, early, 0)
            lax.fori_loop(b_steps + 1, 2 * b_steps, early, 0)

        return carry

    lax.fori_loop(0, n - 1, body, 0)

    dq_copy(lax.rem(me + sign * b_steps + n, n), me).start()
    own_dq = pltpu.make_async_copy(dqs.at[me], dq_out.at[:, columns(me)], own_sem.at[0])
    own_dq.start()

    t = lax.rem(me - sign * a_steps + n, n)
    datt[...] = jnp.zeros(datt.shape, F32)

    def swap(sub):
        part = sub_of(sub)
        return remote(
            wpb.at[half_of(other), part],
            theirs.at[:, part],
            swap_send.at[sub],
            swap_recv.at[sub],
            {"dp_2": other},
        )

    def scatter(d, place_here):
        target, place = chip(d)
        return remote(
            packed.at[place], slots.at[place_here], x_send.at[place], x_recv.at[place_here], target
        )

    def merge(sub):
        swap(sub).wait_recv()

        def piece(j, carry):
            part = pl.ds(pl.multiple_of(j * chunk, chunk), chunk)
            packed[j] = (wpb[half_of(core), part].astype(F32) + theirs[:, part].astype(F32)).astype(BF16)
            return carry

        lax.fori_loop(sub * per_sub, (sub + 1) * per_sub, piece, 0)

    def scatter_of(place):
        return remote(
            packed.at[place],
            slots.at[here],
            x_send.at[place],
            x_recv.at[here],
            {"dp_0": place // side, "dp_1": lax.rem(place, side)},
        )

    def send_sub(sub):
        def one(j, carry):
            place = sub * per_sub + lax.rem(here + j, per_sub)

            @pl.when(place != here)
            def _():
                scatter_of(place).start()

            return carry

        lax.fori_loop(0, per_sub, one, 0)

    for sub in range(SUBS):
        ring(0, a_steps - 1, sub, t, up).wait_recv()
        weigh(t, sub)

        def narrow(j, carry, sub=sub):
            part = pl.ds(pl.multiple_of(sub * quarter + j * 512, 512), 512)
            wpb[:, part] = wacc[:, part].astype(BF16)
            return carry

        lax.fori_loop(0, quarter // 512, narrow, 0)
        if sub > 0:
            merge(sub - 1)
        project(t, sub)
        swap(sub).start()
        if sub > 0:
            send_sub(sub - 1)

    def dkv_copy(i, h, d, place):
        to = peer(d)
        return remote(
            dkv.at[i, rows_of(to), pl.ds(h * HEAD_DIM, HEAD_DIM)],
            (dk_out, dv_out)[i].at[:, pl.ds(pl.multiple_of(place * width + h * HEAD_DIM, HEAD_DIM), HEAD_DIM)],
            dkv_send.at[i, h, d],
            dkv_recv.at[i, h, place],
            {"seq": to},
        )

    for h in range(heads):
        cols = pl.ds(h * HEAD_DIM, HEAD_DIM)
        backward(t, h)

        def finish(j, carry, cols=cols):
            rows = pl.ds(pl.multiple_of(j * 256, 256), 256)
            dkv[1, rows, cols] = jnp.transpose(dvt[cols, rows]).astype(BF16)
            unit, inverse = norm_rows(1, rows, cols)
            d_normed = jnp.transpose(dkt[cols, rows])
            gain[1:2, :] += jnp.sum(unit * d_normed, axis=0, keepdims=True)
            dkv[0, rows, cols] = norm_back(unit, inverse, kg, d_normed)
            return carry

        lax.fori_loop(0, total // 256, finish, 0)
        for i in (1, 0):
            for d in order:
                dkv_copy(i, h, d, me).start()
        if h == 0:
            merge(SUBS - 1)
            send_sub(SUBS - 1)
    dq_copy(t, me).start()
    own_dkv = [
        pltpu.make_async_copy(dkv.at[i, rows_of(me)], out.at[:, columns(me)], own_sem.at[1 + i])
        for i, out in enumerate((dk_out, dv_out))
    ]
    for copy in own_dkv:
        copy.start()

    reduced[...] = packed[here].astype(F32)
    for d in range(1, chips):
        place = chip(d)[1]
        scatter(d, place).wait_recv()
        reduced[...] += slots[place].astype(F32)

    def window(index):
        return pl.ds(pl.multiple_of(index * 128, 128), 256)

    shard_width = chunk // 2
    last = remote(reduced.at[:, window(other)], final, last_send.at[0], last_recv.at[0], {"dp_2": other})
    last.start()

    def pick(block):
        return jnp.where(core == 0, block[:, :shard_width], block[:, 256 - shard_width :])

    mine = pick(reduced[:, window(core)])
    w_out[half_of(core), :] = mine
    square = jnp.sum(mine * mine)
    row = lax.broadcasted_iota(jnp.int32, (8, 128), 0)
    last.wait_recv()
    rest = pick(final[...])
    w_out[half_of(other), :] = rest
    square = square + jnp.sum(rest * rest)
    dp_slots[in_group] = jnp.where(row == 2, square, gain[...])

    def spread(buffer, peers, count, sends, recvs, place):
        def copy(d, source):
            return remote(buffer.at[source], buffer.at[source], sends.at[d], recvs.at[source], peers(d)[0])

        for d in range(1, count):
            copy(d, place).start()
        for d in range(1, count):
            copy(d, peers(d)[1]).wait_recv()
        result = buffer[0]
        for index in range(1, count):
            result = result + buffer[index]
        for d in range(1, count):
            copy(d, place).wait_send()
        return result

    z_slots[me] = spread(dp_slots, dp_peer, group, dp_send, dp_recv, in_group)
    summed = spread(z_slots, z_peer, n, z_send, z_recv, me)
    gains = jnp.where(row < 2, summed, 0.0)
    squares = summed[2:3, 0:1] + jnp.sum(gains * gains)
    norm = jnp.sqrt(squares)
    factor = jnp.minimum(1.0, MAX_NORM / (norm + EPS))
    qgain_out[...] = gains[0:1] * factor
    kgain_out[...] = gains[1:2] * factor
    norm_out[...] = norm
    w_out[...] = w_out[...] * factor

    last.wait_send()
    own_dq.wait()
    for copy in own_dkv:
        copy.wait()
    for i, ref in arrays:
        for d in order:
            qkv_copy(i, ref, d, me).wait_send()
    for sub in range(SUBS):
        swap(sub).wait_send()
        for step in range(a_steps):
            ring(0, step, sub, me, up).wait_send()
        for step in range(b_steps):
            ring(1, step, sub, me, down).wait_send()
    for d in range(1, chips):
        scatter(d, here).wait_send()
    for d in range(1, n):
        dq_copy(peer(d), me).wait_send()
        dq_copy(peer(d), peer(d)).wait_recv()
        for i in (0, 1):
            for h in range(heads):
                dkv_copy(i, h, d, me).wait_send()
                dkv_copy(i, h, d, peer(d)).wait_recv()


def write_kernel(dq_in, dk_in, dv_in, w_in, qgain_in, kgain_in, norm_in, dq_out, dk_out, dv_out, w_out, qgain_out, kgain_out, norm_out, held, in_sem, out_sem):
    pieces = held.shape[1]
    rows = held.shape[2]
    refs = ((dq_in, dq_out), (dk_in, dk_out), (dv_in, dv_out))

    def load(i, p):
        return pltpu.make_async_copy(refs[i][0].at[pl.ds(p * rows, rows)], held.at[i, p], in_sem.at[i, p])

    def store(i, p):
        return pltpu.make_async_copy(held.at[i, p], refs[i][1].at[pl.ds(p * rows, rows)], out_sem.at[i, p])

    every = [(i, p) for i in range(3) for p in range(pieces)]
    for i, p in every:
        load(i, p).start()
    w_out[...] = jnp.transpose(w_in[...])
    qgain_out[...] = qgain_in[...]
    kgain_out[...] = kgain_in[...]
    norm_out[...] = norm_in[...]
    for i, p in every:
        load(i, p).wait()
        store(i, p).start()
    for i, p in every:
        store(i, p).wait()


def local(n, side, query_rows, key_rows, value_rows, out_grad, clip_lengths, out_weight, query_gain, key_gain):
    tokens, inner = query_rows.shape[1:]
    model = out_grad.shape[2]
    width = inner // n
    heads = width // HEAD_DIM
    total = tokens * n
    vmem = pl.BlockSpec(memory_space=pltpu.VMEM)
    smem = pl.BlockSpec(memory_space=pltpu.SMEM)
    anywhere = pl.BlockSpec(memory_space=pl.ANY)
    dma = pltpu.SemaphoreType.DMA
    struct = jax.ShapeDtypeStruct
    chips = side * side
    chunk = model // chips
    dq, dk, dv, weight_grad, qgain, kgain, norm = pl.pallas_call(
        functools.partial(kernel, n, side),
        out_shape=(
            struct((tokens, inner), BF16),
            struct((tokens, inner), BF16),
            struct((tokens, inner), BF16),
            struct((width, chunk // 2), F32),
            struct((1, HEAD_DIM), F32),
            struct((1, HEAD_DIM), F32),
            struct((1, 1), F32),
        ),
        in_specs=[anywhere] * 5 + [smem, vmem, vmem],
        out_specs=(anywhere, anywhere, anywhere, vmem, vmem, vmem, vmem),
        scratch_shapes=[
            pltpu.VMEM((3, total, width), BF16),
            pltpu.VMEM((total, width), BF16),
            pltpu.VMEM((width, total), BF16),
            pltpu.VMEM((width, total), BF16),
            pltpu.VMEM((n, SUBS, tokens, model // SUBS), BF16),
            pltpu.VMEM((width, model), BF16),
            pltpu.VMEM((width, model), F32),
            pltpu.VMEM((width, total), F32),
            pltpu.VMEM((width, total), F32),
            pltpu.VMEM((tokens, width), F32),
            pltpu.VMEM((width, total), BF16),
            pltpu.VMEM((heads, total, total), BF16),
            pltpu.VMEM((n, tokens, width), BF16),
            pltpu.VMEM((2, total, width), BF16),
            pltpu.VMEM((8, HEAD_DIM), F32),
            pltpu.VMEM((width, model), BF16),
            pltpu.VMEM((width // 2, model), BF16),
            pltpu.VMEM((chips, width // 2, chunk), BF16),
            pltpu.VMEM((chips, width // 2, chunk), BF16),
            pltpu.VMEM((width // 2, chunk), F32),
            pltpu.VMEM((width // 2, 256), F32),
            pltpu.VMEM((n, 8, 128), F32),
            pltpu.VMEM((2 * chips, 8, 128), F32),
            dma((3, n)),
            dma((3, n)),
            dma((2, n // 2, SUBS)),
            dma((n, SUBS)),
            dma((n,)),
            dma((n,)),
            dma((2, heads, n)),
            dma((2, heads, n)),
            dma((SUBS,)),
            dma((SUBS,)),
            dma((chips,)),
            dma((chips,)),
            dma((1,)),
            dma((1,)),
            dma((n,)),
            dma((n,)),
            dma((2 * chips,)),
            dma((2 * chips,)),
            dma((8,)),
        ],
        compiler_params=pltpu.CompilerParams(
            collective_id=1, has_side_effects=True, vmem_limit_bytes=67043328
        ),
        name="fused",
    )(
        query_rows[0],
        key_rows[0],
        value_rows[0],
        out_grad[0],
        out_weight,
        clip_lengths[0],
        query_gain[None],
        key_gain[None],
    )
    rows = struct((tokens, inner), BF16)
    gain = struct((1, HEAD_DIM), F32)
    dq, dk, dv, weight_grad, qgain, kgain, norm = pl.pallas_call(
        write_kernel,
        out_shape=(rows, rows, rows, struct((chunk // 2, width), F32), gain, gain, struct((1, 1), F32)),
        in_specs=[anywhere] * 3 + [vmem] * 4,
        out_specs=(anywhere, anywhere, anywhere, vmem, vmem, vmem, vmem),
        scratch_shapes=[pltpu.VMEM((3, 2, tokens // 2, inner), BF16), dma((3, 2)), dma((3, 2))],
        name="write",
    )(dq, dk, dv, weight_grad, qgain, kgain, norm)
    return (
        dq[None],
        dk[None],
        dv[None],
        weight_grad.T,
        qgain.reshape(HEAD_DIM),
        kgain.reshape(HEAD_DIM),
        norm.reshape(()),
    )


def solution(mesh):
    n = mesh.shape["seq"]
    torus = Mesh(mesh.devices.reshape(4, 4, 2, n), ("dp_0", "dp_1", "dp_2", "seq"))
    return jax.shard_map(
        functools.partial(local, n, 4),
        mesh=torus,
        in_specs=(
            P(DP, "seq", None),
            P(DP, "seq", None),
            P(DP, "seq", None),
            P(DP, "seq", None),
            P(DP, None),
            P("seq", None),
            P(),
            P(),
        ),
        out_specs=(
            P(DP, "seq", None),
            P(DP, "seq", None),
            P(DP, "seq", None),
            P("seq", DP),
            P(),
            P(),
            P(),
        ),
        check_vma=False,
    )
```

```python
import functools

import jax
import jax.numpy as jnp
from jax import lax
from jax.experimental import pallas as pl
from jax.experimental.pallas import tpu as pltpu
from jax.sharding import Mesh
from jax.sharding import PartitionSpec as P

HEAD_DIM = 128
MAX_NORM = 768
EPS = 1e-06
DP = ("dp_0", "dp_1", "dp_2")
MESH = pl.DeviceIdType.MESH
F32 = jnp.float32
BF16 = jnp.bfloat16
NN = (((1,), (0,)), ((), ()))
NT = (((1,), (1,)), ((), ()))
SUBS = 4


def dot(a, b, dims=NN):
    return lax.dot_general(a, b, dims, preferred_element_type=F32)


def seg_of(places, lengths_ref):
    seg = jnp.zeros(places.shape, jnp.int32)
    end = jnp.int32(0)
    for c in range(lengths_ref.shape[0]):
        end = end + lengths_ref[c]
        seg = seg + (places >= end).astype(jnp.int32)
    return seg


def kernel(
    n,
    side,
    q_hbm,
    k_hbm,
    v_hbm,
    do_hbm,
    w_hbm,
    lengths_ref,
    qg_ref,
    kg_ref,
    dq_out,
    dk_out,
    dv_out,
    w_out,
    small_out,
    qkv,
    kn,
    knt,
    vt,
    do_all,
    w,
    wacc,
    dkt,
    dvt,
    datt,
    attnt,
    probs,
    dqs,
    dkv,
    gain,
    wpb,
    theirs,
    packed,
    slots,
    part,
    second,
    reduced,
    final,
    z_slots,
    row_slots,
    y_slots,
    qkv_send,
    qkv_recv,
    ag_send,
    ag_recv,
    dq_send,
    dq_recv,
    dkv_send,
    dkv_recv,
    swap_send,
    swap_recv,
    first_send,
    first_recv,
    second_send,
    second_recv,
    last_send,
    last_recv,
    z_send,
    z_recv,
    row_send,
    row_recv,
    y_send,
    y_recv,
    own_sem,
):
    me = lax.axis_index("seq")
    y, x, core = (lax.axis_index(name) for name in DP)
    other = 1 - core
    sign = 1 - 2 * core
    tokens = q_hbm.shape[0]
    total = tokens * n
    width = q_hbm.shape[1] // n
    heads = width // HEAD_DIM
    model = do_hbm.shape[1]
    quarter = model // SUBS
    scale = HEAD_DIM ** (-0.5)
    up = lax.rem(me + sign + n, n)
    down = lax.rem(me - sign + n, n)
    a_steps = n // 2
    b_steps = n - 1 - a_steps
    chips = side * side
    chunk = model // chips
    per_sub = chips // SUBS
    half = width // 2
    in_row = x * 2 + core
    home = lax.rem(x + y, side)

    def columns(index):
        return pl.ds(pl.multiple_of(index * width, width), width)

    def rows_of(index):
        return pl.ds(pl.multiple_of(index * tokens, tokens), tokens)

    def half_of(index):
        return pl.ds(pl.multiple_of(index * half, half), half)

    def sub_of(index):
        return pl.ds(index * quarter, quarter)

    def peer(d):
        return lax.rem(me + d, n)

    def z_peer(d):
        return {"seq": peer(d)}, peer(d)

    def row_peer(d):
        place = lax.rem(in_row + d, 2 * side)
        return {"dp_1": place // 2, "dp_2": lax.rem(place, 2)}, place

    def y_peer(d):
        place = lax.rem(y + d, side)
        return {"dp_0": place}, place

    def x_peer(d):
        place = lax.rem(x + d, side)
        return {"dp_1": place}, place

    def remote(src, dst, send, recv, to):
        return pltpu.make_async_remote_copy(
            src_ref=src, dst_ref=dst, send_sem=send, recv_sem=recv, device_id=to, device_id_type=MESH
        )

    barrier = pltpu.get_barrier_semaphore()
    for d in range(1, n):
        pl.semaphore_signal(barrier, inc=1, device_id=z_peer(d)[0], device_id_type=MESH)
    for d in range(1, 2 * side):
        pl.semaphore_signal(barrier, inc=1, device_id=row_peer(d)[0], device_id_type=MESH)
    for d in range(1, side):
        pl.semaphore_signal(barrier, inc=1, device_id=y_peer(d)[0], device_id_type=MESH)

    own_copies = [
        pltpu.make_async_copy(ref.at[:, columns(me)], qkv.at[i, rows_of(me)], own_sem.at[i])
        for i, ref in enumerate((q_hbm, k_hbm, v_hbm))
    ]
    def chunk_at(sub, j):
        return side * j + lax.rem(sub - j + side, side)

    def chunk_of(index):
        return pl.ds(pl.multiple_of(index * chunk, chunk), chunk)

    do_copies = [
        pltpu.make_async_copy(
            do_hbm.at[:, chunk_of(chunk_at(sub, j))],
            do_all.at[me, sub, :, pl.ds(j * chunk, chunk)],
            own_sem.at[4 + sub * per_sub + j],
        )
        for sub in range(SUBS)
        for j in range(per_sub)
    ]
    w_copies = [
        pltpu.make_async_copy(
            w_hbm.at[:, chunk_of(chunk_at(sub, j))],
            w.at[:, pl.ds((sub * per_sub + j) * chunk, chunk)],
            own_sem.at[4 + chips + sub * per_sub + j],
        )
        for sub in range(SUBS)
        for j in range(per_sub)
    ]
    for copy in do_copies + own_copies + w_copies:
        copy.start()
    pl.semaphore_wait(barrier, n + 3 * side - 3)

    order = [4, 3, 5, 2, 6, 1, 7] if n == 8 else list(range(1, n))
    arrays = ((1, k_hbm), (2, v_hbm), (0, q_hbm))

    def qkv_copy(i, ref, d, place):
        to = peer(d)
        return remote(
            ref.at[:, columns(to)],
            qkv.at[i, rows_of(place)],
            qkv_send.at[i, d],
            qkv_recv.at[i, place],
            {"seq": to},
        )

    for i, ref in arrays:
        for d in order:
            qkv_copy(i, ref, d, me).start()

    def ring(direction, step, sub, block, to):
        return remote(
            do_all.at[block, sub],
            do_all.at[block, sub],
            ag_send.at[direction, step, sub],
            ag_recv.at[block, sub],
            {"seq": to},
        )

    for copy in do_copies:
        copy.wait()
    for sub in range(SUBS):
        ring(0, 0, sub, me, up).start()
        ring(1, 0, sub, me, down).start()

    dkt[...] = jnp.zeros(dkt.shape, F32)
    dvt[...] = jnp.zeros(dvt.shape, F32)
    gain[...] = jnp.zeros(gain.shape, F32)

    def clear(i, carry):
        wacc[:, pl.ds(pl.multiple_of(i * 512, 512), 512)] = jnp.zeros((width, 512), F32)
        return carry

    lax.fori_loop(0, model // 512, clear, 0)
    kg = kg_ref[...]
    qg = qg_ref[...]
    seg_k = seg_of(lax.broadcasted_iota(jnp.int32, (1, total), 1), lengths_ref)

    def project(t, sub):
        term = dot(do_all[t, sub], w[:, sub_of(sub)], NT)
        datt[t] = term if sub == 0 else datt[t] + term

    for copy in w_copies:
        copy.wait()
    for sub in range(SUBS):
        project(me, sub)
    for copy in own_copies:
        copy.wait()
    for i, ref in arrays:
        for d in range(1, n):
            qkv_copy(i, ref, d, peer(d)).wait_recv()

    def norm_rows(i, rows, cols):
        block = qkv[i, rows, cols].astype(F32)
        inverse = lax.rsqrt(jnp.mean(block * block, axis=-1, keepdims=True) + EPS)
        return block * inverse, inverse

    def norm_back(unit, inverse, weight, d_normed):
        d_unit = d_normed * weight
        d_rows = inverse * (d_unit - unit * jnp.mean(unit * d_unit, axis=-1, keepdims=True))
        return d_rows.astype(BF16)

    for h in range(heads):
        cols = pl.ds(h * HEAD_DIM, HEAD_DIM)

        def prepare(j, carry, cols=cols):
            rows = pl.ds(pl.multiple_of(j * 256, 256), 256)
            normed = norm_rows(1, rows, cols)[0] * kg
            kn[rows, cols] = normed.astype(BF16)
            knt[cols, rows] = jnp.transpose(normed).astype(BF16)
            vt[cols, rows] = jnp.transpose(qkv[2, rows, cols].astype(F32)).astype(BF16)
            return carry

        lax.fori_loop(0, total // 256, prepare, 0)

    def forward(j, carry):
        rows = pl.ds(pl.multiple_of(j * 256, 256), 256)
        places = lax.broadcasted_iota(jnp.int32, (256, 1), 0) + j * 256
        same = seg_of(places, lengths_ref) == seg_k
        for h in range(heads):
            cols = pl.ds(h * HEAD_DIM, HEAD_DIM)
            qn = (norm_rows(0, rows, cols)[0] * qg).astype(BF16)
            expo = jnp.where(same, jnp.exp(dot(qn, knt[cols, :]) * scale), 0.0)
            prob = (expo * (1.0 / jnp.sum(expo, axis=-1, keepdims=True))).astype(BF16)
            probs[h, rows, :] = prob
            attn = dot(prob, qkv[2, :, cols])
            attnt[cols, rows] = jnp.transpose(attn).astype(BF16)
        return carry

    lax.fori_loop(0, total // 256, forward, 0)

    def weigh(t, sub):
        def piece(j, c):
            part = pl.ds(pl.multiple_of(j * 512, 512), 512)
            into = pl.ds(pl.multiple_of(sub * quarter + j * 512, 512), 512)
            wacc[:, into] += dot(attnt[:, rows_of(t)], do_all[t, sub, :, part])
            return c

        lax.fori_loop(0, quarter // 512, piece, 0)

    def backward(t, h):
        rows = rows_of(t)
        cols = pl.ds(h * HEAD_DIM, HEAD_DIM)
        unit, inverse = norm_rows(0, rows, cols)
        normed = unit * qg
        dattn = datt[t, :, cols]
        prob = probs[h, rows, :]
        prob32 = prob.astype(F32)
        d_probs = dot(dattn.astype(BF16), vt[cols, :])
        row_sum = jnp.sum(prob32 * d_probs, axis=-1, keepdims=True)
        d_scores = (prob32 * (d_probs - row_sum) * scale).astype(BF16)
        dvt[cols, :] += dot(jnp.transpose(dattn).astype(BF16), prob)
        dkt[cols, :] += dot(jnp.transpose(normed).astype(BF16), d_scores)
        d_normed = dot(d_scores, kn[:, cols])
        gain[0:1, :] += jnp.sum(unit * d_normed, axis=0, keepdims=True)
        dqs[t, :, cols] = norm_back(unit, inverse, qg, d_normed)

    def dq_copy(t, place):
        return remote(
            dqs.at[t], dq_out.at[:, columns(place)], dq_send.at[t], dq_recv.at[place], {"seq": t}
        )

    def block_at(shift):
        return lax.rem(me + sign * shift + n, n)

    for sub in range(SUBS):
        weigh(me, sub)

    def body(step, carry):
        a_block = block_at(-step)
        b_block = block_at(step)
        a_last = block_at(1 - step)
        b_last = block_at(step - 1)
        for sub in range(SUBS):
            ring(0, step - 1, sub, a_block, up).wait_recv()
            ring(0, step, sub, a_block, up).start()
            ring(1, step - 1, sub, b_block, down).wait_recv()

            @pl.when(step < b_steps)
            def _():
                ring(1, step, sub, b_block, down).start()

            for block in (a_block, b_block):
                project(block, sub)
                weigh(block, sub)
            if sub == 0:
                backward(a_last, 0)
            elif sub == 1:
                for h in range(1, heads):
                    backward(a_last, h)
            else:

                @pl.when(step > 1)
                def _():
                    for h in (0,) if sub == 2 else range(1, heads):
                        backward(b_last, h)

        return carry

    lax.fori_loop(1, a_steps, body, 0)
    own_dq = pltpu.make_async_copy(dqs.at[me], dq_out.at[:, columns(me)], own_sem.at[0])
    own_dq.start()

    t = block_at(-a_steps)
    a_last = block_at(-b_steps)
    b_last = block_at(b_steps)

    def swap(sub):
        part = sub_of(sub)
        return remote(
            wpb.at[half_of(other), part],
            theirs.at[:, part],
            swap_send.at[sub],
            swap_recv.at[sub],
            {"dp_2": other},
        )

    def held_at(sub, place):
        return chunk_at(sub, lax.rem(sub - place + side, side)) if sub % 2 == 0 else chunk_at(sub, place)

    def first_copy(sub, d, source):
        to, place = x_peer(d) if sub % 2 == 0 else y_peer(d)
        return remote(
            packed.at[held_at(sub, place)],
            slots.at[sub, source],
            first_send.at[sub, d],
            first_recv.at[sub, source],
            to,
        )

    def first_sends(sub):
        for d in range(1, side):
            first_copy(sub, d, x if sub % 2 == 0 else y).start()

    def second_copy(sub):
        owner = lax.rem(sub - (x if sub % 2 == 0 else y) + side, side)
        source = y if sub % 2 == 0 else x
        return remote(
            part.at[sub],
            second.at[source],
            second_send.at[sub],
            second_recv.at[source],
            {"dp_0": owner} if sub % 2 == 0 else {"dp_1": owner},
        )

    def combine(sub):
        whole = packed[held_at(sub, x if sub % 2 == 0 else y)].astype(F32)
        for d in range(1, side):
            source = (x_peer(d) if sub % 2 == 0 else y_peer(d))[1]
            first_copy(sub, d, source).wait_recv()
            whole = whole + slots[sub, source].astype(F32)
        part[sub] = whole.astype(BF16)

    def second_sends(sub):
        @pl.when(home != sub)
        def _():
            second_copy(sub).start()

    def merge(sub):
        swap(sub).wait_recv()

        def piece(j, carry):
            part = chunk_of(sub * per_sub + j)
            whole = wpb[half_of(core), part].astype(F32) + theirs[:, part].astype(F32)
            packed[chunk_at(sub, j)] = whole.astype(BF16)
            return carry

        lax.fori_loop(0, per_sub, piece, 0)

    for sub in range(SUBS):
        ring(0, a_steps - 1, sub, t, up).wait_recv()
        if sub == SUBS - 1:
            for step in range(1, b_steps):
                dq_copy(block_at(-step), me).start()
                dq_copy(block_at(step), me).start()
            dq_copy(a_last, me).start()
        weigh(t, sub)

        def narrow(j, carry, sub=sub):
            part = pl.ds(pl.multiple_of(sub * quarter + j * 512, 512), 512)
            wpb[:, part] = wacc[:, part].astype(BF16)
            return carry

        lax.fori_loop(0, quarter // 512, narrow, 0)
        swap(sub).start()
        project(t, sub)
        merge(sub)
        first_sends(sub)
        if sub > 0:
            combine(sub - 1)
            second_sends(sub - 1)
        if sub < heads:
            backward(a_last, sub)
    def dkv_copy(i, h, d, place):
        to = peer(d)
        return remote(
            dkv.at[i, rows_of(to), pl.ds(h * HEAD_DIM, HEAD_DIM)],
            (dk_out, dv_out)[i].at[:, pl.ds(pl.multiple_of(place * width + h * HEAD_DIM, HEAD_DIM), HEAD_DIM)],
            dkv_send.at[i, h, d],
            dkv_recv.at[i, h, place],
            {"seq": to},
        )

    for h in range(heads):
        cols = pl.ds(h * HEAD_DIM, HEAD_DIM)
        backward(b_last, h)
        backward(t, h)

        def finish(j, carry, cols=cols):
            rows = pl.ds(pl.multiple_of(j * 256, 256), 256)
            dkv[1, rows, cols] = jnp.transpose(dvt[cols, rows]).astype(BF16)
            unit, inverse = norm_rows(1, rows, cols)
            d_normed = jnp.transpose(dkt[cols, rows])
            gain[1:2, :] += jnp.sum(unit * d_normed, axis=0, keepdims=True)
            dkv[0, rows, cols] = norm_back(unit, inverse, kg, d_normed)
            return carry

        lax.fori_loop(0, total // 256, finish, 0)
        for i in (1, 0) if h < heads - 1 else (1,):
            for d in order:
                dkv_copy(i, h, d, me).start()
        if h == 0:
            combine(SUBS - 1)
            second_sends(SUBS - 1)
    dq_copy(b_last, me).start()
    dq_copy(t, me).start()
    own_dkv = [
        pltpu.make_async_copy(dkv.at[i, rows_of(me)], out.at[:, columns(me)], own_sem.at[1 + i])
        for i, out in enumerate((dk_out, dv_out))
    ]
    for copy in own_dkv:
        copy.start()

    reduced[...] = part[home].astype(F32)
    start = jnp.where(lax.rem(home, 2) == 0, y, x)
    for d in range(1, side):
        source = lax.rem(start + d, side)
        remote(part.at[0], second.at[source], second_send.at[0], second_recv.at[source], x_peer(1)[0]).wait_recv()
        reduced[...] += second[source].astype(F32)

    def window(index):
        return pl.ds(pl.multiple_of(index * 128, 128), 256)

    shard_width = chunk // 2
    last = remote(reduced.at[:, window(other)], final, last_send.at[0], last_recv.at[0], {"dp_2": other})
    last.start()

    def pick(block):
        return jnp.where(core == 0, block[:, :shard_width], block[:, 256 - shard_width :])

    square = jnp.sum(reduced[...] * reduced[...])
    row = lax.broadcasted_iota(jnp.int32, (8, 128), 0)
    row_slots[in_row] = jnp.where(row == 2, square, gain[...])
    w_out[half_of(core), :] = pick(reduced[:, window(core)])

    def rest_of_dk():
        for d in order:
            dkv_copy(0, heads - 1, d, me).start()

    def spread(buffer, peers, count, sends, recvs, place, then=None):
        def copy(d, source):
            return remote(buffer.at[source], buffer.at[source], sends.at[d], recvs.at[source], peers(d)[0])

        for d in range(1, count):
            copy(d, place).start()
        if then is not None:
            then()
        for d in range(1, count):
            copy(d, peers(d)[1]).wait_recv()
        result = buffer[0]
        for index in range(1, count):
            result = result + buffer[index]
        for d in range(1, count):
            copy(d, place).wait_send()
        return result

    y_slots[y] = spread(row_slots, row_peer, 2 * side, row_send, row_recv, in_row)
    z_slots[me] = spread(y_slots, y_peer, side, y_send, y_recv, y)
    last.wait_recv()
    w_out[half_of(other), :] = pick(final[...])
    summed = spread(z_slots, z_peer, n, z_send, z_recv, me, rest_of_dk)
    gains = jnp.where(row < 2, summed, 0.0)
    squares = summed[2:3, 0:1] + jnp.sum(gains * gains)
    norm = jnp.sqrt(squares)
    factor = jnp.minimum(1.0, MAX_NORM / (norm + EPS))
    small_out[...] = jnp.where(row < 2, gains * factor, norm)
    w_out[...] = w_out[...] * factor

    last.wait_send()
    own_dq.wait()
    for copy in own_dkv:
        copy.wait()
    for i, ref in arrays:
        for d in order:
            qkv_copy(i, ref, d, me).wait_send()
    for sub in range(SUBS):
        swap(sub).wait_send()
        for step in range(a_steps):
            ring(0, step, sub, me, up).wait_send()
        for step in range(b_steps):
            ring(1, step, sub, me, down).wait_send()
        for d in range(1, side):
            first_copy(sub, d, 0).wait_send()

        @pl.when(home != sub)
        def _():
            second_copy(sub).wait_send()

    for d in range(1, n):
        dq_copy(peer(d), me).wait_send()
        dq_copy(peer(d), peer(d)).wait_recv()
        for i in (0, 1):
            for h in range(heads):
                dkv_copy(i, h, d, me).wait_send()
                dkv_copy(i, h, d, peer(d)).wait_recv()


def write_kernel(
    dq_in, dk_in, dv_in, w_in, small_in, dq_out, dk_out, dv_out, w_out, qgain_out, kgain_out, norm_out,
    rows, block, turned, small, norm, in_sem, out_sem,
):
    loads = [pltpu.make_async_copy(w_in, block, in_sem.at[3]), pltpu.make_async_copy(small_in, small, in_sem.at[4])]
    for i, ref in enumerate((dq_in, dk_in, dv_in)):
        loads.append(pltpu.make_async_copy(ref, rows.at[i], in_sem.at[i]))
    for load in loads:
        load.start()
    stores = [
        pltpu.make_async_copy(small.at[0:1], qgain_out, out_sem.at[3]),
        pltpu.make_async_copy(small.at[1:2], kgain_out, out_sem.at[4]),
        pltpu.make_async_copy(norm, norm_out, out_sem.at[5]),
        pltpu.make_async_copy(turned, w_out, out_sem.at[6]),
    ]
    loads[0].wait()
    loads[1].wait()
    norm[...] = small[2:3, :]
    turned[...] = jnp.transpose(block[...])
    for i, ref in enumerate((dq_out, dk_out, dv_out)):
        loads[2 + i].wait()
        stores.append(pltpu.make_async_copy(rows.at[i], ref, out_sem.at[i]))
        stores[-1].start()
    for store in stores[:4]:
        store.start()
    for store in stores:
        store.wait()


def local(n, side, query_rows, key_rows, value_rows, out_grad, clip_lengths, out_weight, query_gain, key_gain):
    tokens, inner = query_rows.shape[1:]
    model = out_grad.shape[2]
    width = inner // n
    heads = width // HEAD_DIM
    total = tokens * n
    vmem = pl.BlockSpec(memory_space=pltpu.VMEM)
    smem = pl.BlockSpec(memory_space=pltpu.SMEM)
    anywhere = pl.BlockSpec(memory_space=pl.ANY)
    dma = pltpu.SemaphoreType.DMA
    struct = jax.ShapeDtypeStruct
    chips = side * side
    chunk = model // chips
    dq, dk, dv, weight_grad, small = pl.pallas_call(
        functools.partial(kernel, n, side),
        out_shape=(
            struct((tokens, inner), BF16),
            struct((tokens, inner), BF16),
            struct((tokens, inner), BF16),
            struct((width, chunk // 2), F32),
            struct((8, HEAD_DIM), F32),
        ),
        in_specs=[anywhere] * 5 + [smem, vmem, vmem],
        out_specs=(anywhere, anywhere, anywhere, vmem, vmem),
        scratch_shapes=[
            pltpu.VMEM((3, total, width), BF16),
            pltpu.VMEM((total, width), BF16),
            pltpu.VMEM((width, total), BF16),
            pltpu.VMEM((width, total), BF16),
            pltpu.VMEM((n, SUBS, tokens, model // SUBS), BF16),
            pltpu.VMEM((width, model), BF16),
            pltpu.VMEM((width, model), F32),
            pltpu.VMEM((width, total), F32),
            pltpu.VMEM((width, total), F32),
            pltpu.VMEM((n, tokens, width), F32),
            pltpu.VMEM((width, total), BF16),
            pltpu.VMEM((heads, total, total), BF16),
            pltpu.VMEM((n, tokens, width), BF16),
            pltpu.VMEM((2, total, width), BF16),
            pltpu.VMEM((8, HEAD_DIM), F32),
            pltpu.VMEM((width, model), BF16),
            pltpu.VMEM((width // 2, model), BF16),
            pltpu.VMEM((chips, width // 2, chunk), BF16),
            pltpu.VMEM((SUBS, side, width // 2, chunk), BF16),
            pltpu.VMEM((SUBS, width // 2, chunk), BF16),
            pltpu.VMEM((side, width // 2, chunk), BF16),
            pltpu.VMEM((width // 2, chunk), F32),
            pltpu.VMEM((width // 2, 256), F32),
            pltpu.VMEM((n, 8, 128), F32),
            pltpu.VMEM((2 * side, 8, 128), F32),
            pltpu.VMEM((side, 8, 128), F32),
            dma((3, n)),
            dma((3, n)),
            dma((2, n // 2, SUBS)),
            dma((n, SUBS)),
            dma((n,)),
            dma((n,)),
            dma((2, heads, n)),
            dma((2, heads, n)),
            dma((SUBS,)),
            dma((SUBS,)),
            dma((SUBS, side)),
            dma((SUBS, side)),
            dma((SUBS,)),
            dma((side,)),
            dma((1,)),
            dma((1,)),
            dma((n,)),
            dma((n,)),
            dma((2 * side,)),
            dma((2 * side,)),
            dma((side,)),
            dma((side,)),
            dma((4 + 2 * chips,)),
        ],
        compiler_params=pltpu.CompilerParams(
            collective_id=1, has_side_effects=True, vmem_limit_bytes=67043328
        ),
        name="fused",
    )(
        query_rows[0],
        key_rows[0],
        value_rows[0],
        out_grad[0],
        out_weight,
        clip_lengths[0],
        query_gain[None],
        key_gain[None],
    )
    rows = struct((tokens, inner), BF16)
    gain = struct((1, HEAD_DIM), F32)
    dq, dk, dv, weight_grad, qgain, kgain, norm = pl.pallas_call(
        write_kernel,
        out_shape=(rows, rows, rows, struct((chunk // 2, width), F32), gain, gain, gain),
        in_specs=[anywhere] * 5,
        out_specs=(anywhere,) * 7,
        scratch_shapes=[
            pltpu.VMEM((3, tokens, inner), BF16),
            pltpu.VMEM((width, chunk // 2), F32),
            pltpu.VMEM((chunk // 2, width), F32),
            pltpu.VMEM((8, HEAD_DIM), F32),
            pltpu.VMEM((1, HEAD_DIM), F32),
            dma((5,)),
            dma((7,)),
        ],
        name="write",
    )(dq, dk, dv, weight_grad, small)
    return (
        dq[None],
        dk[None],
        dv[None],
        weight_grad.T,
        qgain.reshape(HEAD_DIM),
        kgain.reshape(HEAD_DIM),
        norm[0, 0],
    )


def solution(mesh):
    n = mesh.shape["seq"]
    torus = Mesh(mesh.devices.reshape(4, 4, 2, n), ("dp_0", "dp_1", "dp_2", "seq"))
    return jax.shard_map(
        functools.partial(local, n, 4),
        mesh=torus,
        in_specs=(
            P(DP, "seq", None),
            P(DP, "seq", None),
            P(DP, "seq", None),
            P(DP, "seq", None),
            P(DP, None),
            P("seq", None),
            P(),
            P(),
        ),
        out_specs=(
            P(DP, "seq", None),
            P(DP, "seq", None),
            P(DP, "seq", None),
            P("seq", DP),
            P(),
            P(),
            P(),
        ),
        check_vma=False,
    )
```

```python
import functools

import jax
import jax.numpy as jnp
from jax import lax
from jax.experimental import pallas as pl
from jax.experimental.pallas import tpu as pltpu
from jax.sharding import Mesh
from jax.sharding import PartitionSpec as P

HEAD_DIM = 128
MAX_NORM = 768
EPS = 1e-06
DP = ("dp_0", "dp_1", "dp_2")
MESH = pl.DeviceIdType.MESH
F32 = jnp.float32
BF16 = jnp.bfloat16
NN = (((1,), (0,)), ((), ()))
NT = (((1,), (1,)), ((), ()))
SUBS = 4


def dot(a, b, dims=NN):
    return lax.dot_general(a, b, dims, preferred_element_type=F32)


def seg_of(places, lengths_ref):
    seg = jnp.zeros(places.shape, jnp.int32)
    end = jnp.int32(0)
    for c in range(lengths_ref.shape[0]):
        end = end + lengths_ref[c]
        seg = seg + (places >= end).astype(jnp.int32)
    return seg


def kernel(
    n,
    side,
    q_hbm,
    k_hbm,
    v_hbm,
    do_hbm,
    w_hbm,
    lengths_hbm,
    qg_hbm,
    kg_hbm,
    dq_out,
    dk_out,
    dv_out,
    w_hbm_out,
    small_hbm_out,
    lengths_ref,
    gains_in,
    w_out,
    small_out,
    qkv,
    kn,
    knt,
    vt,
    do_all,
    w,
    wacc,
    dkt,
    dvt,
    datt,
    attnt,
    probs,
    dqs,
    dkv,
    gain,
    wpb,
    theirs,
    packed,
    slots,
    part,
    second,
    reduced,
    final,
    z_slots,
    row_slots,
    y_slots,
    qkv_send,
    qkv_recv,
    ag_send,
    ag_recv,
    dq_send,
    dq_recv,
    dkv_send,
    dkv_recv,
    swap_send,
    swap_recv,
    first_send,
    first_recv,
    second_send,
    second_recv,
    last_send,
    last_recv,
    z_send,
    z_recv,
    row_send,
    row_recv,
    y_send,
    y_recv,
    own_sem,
):
    me = lax.axis_index("seq")
    y, x, core = (lax.axis_index(name) for name in DP)
    other = 1 - core
    sign = 1 - 2 * core
    tokens = q_hbm.shape[0]
    total = tokens * n
    width = q_hbm.shape[1] // n
    heads = width // HEAD_DIM
    model = do_hbm.shape[1]
    quarter = model // SUBS
    scale = HEAD_DIM ** (-0.5)
    up = lax.rem(me + sign + n, n)
    down = lax.rem(me - sign + n, n)
    a_steps = n // 2
    b_steps = n - 1 - a_steps
    chips = side * side
    chunk = model // chips
    per_sub = chips // SUBS
    half = width // 2
    in_row = x * 2 + core
    home = lax.rem(x + y, side)

    def columns(index):
        return pl.ds(pl.multiple_of(index * width, width), width)

    def rows_of(index):
        return pl.ds(pl.multiple_of(index * tokens, tokens), tokens)

    def half_of(index):
        return pl.ds(pl.multiple_of(index * half, half), half)

    def sub_of(index):
        return pl.ds(index * quarter, quarter)

    def peer(d):
        return lax.rem(me + d, n)

    def z_peer(d):
        return {"seq": peer(d)}, peer(d)

    def row_peer(d):
        place = lax.rem(in_row + d, 2 * side)
        return {"dp_1": place // 2, "dp_2": lax.rem(place, 2)}, place

    def y_peer(d):
        place = lax.rem(y + d, side)
        return {"dp_0": place}, place

    def x_peer(d):
        place = lax.rem(x + d, side)
        return {"dp_1": place}, place

    def remote(src, dst, send, recv, to):
        return pltpu.make_async_remote_copy(
            src_ref=src, dst_ref=dst, send_sem=send, recv_sem=recv, device_id=to, device_id_type=MESH
        )

    barrier = pltpu.get_barrier_semaphore()
    for d in range(1, n):
        pl.semaphore_signal(barrier, inc=1, device_id=z_peer(d)[0], device_id_type=MESH)
    for d in range(1, 2 * side):
        pl.semaphore_signal(barrier, inc=1, device_id=row_peer(d)[0], device_id_type=MESH)
    for d in range(1, side):
        pl.semaphore_signal(barrier, inc=1, device_id=y_peer(d)[0], device_id_type=MESH)

    own_copies = [
        pltpu.make_async_copy(ref.at[:, columns(me)], qkv.at[i, rows_of(me)], own_sem.at[i])
        for i, ref in enumerate((q_hbm, k_hbm, v_hbm))
    ]
    def chunk_at(sub, j):
        return side * j + lax.rem(sub - j + side, side)

    def chunk_of(index):
        return pl.ds(pl.multiple_of(index * chunk, chunk), chunk)

    do_copies = [
        pltpu.make_async_copy(
            do_hbm.at[:, chunk_of(chunk_at(sub, j))],
            do_all.at[me, sub, :, pl.ds(j * chunk, chunk)],
            own_sem.at[4 + sub * per_sub + j],
        )
        for sub in range(SUBS)
        for j in range(per_sub)
    ]
    w_copies = [
        pltpu.make_async_copy(
            w_hbm.at[:, chunk_of(chunk_at(sub, j))],
            w.at[:, pl.ds((sub * per_sub + j) * chunk, chunk)],
            own_sem.at[4 + chips + sub * per_sub + j],
        )
        for sub in range(SUBS)
        for j in range(per_sub)
    ]
    small_copies = [
        pltpu.make_async_copy(lengths_hbm, lengths_ref, own_sem.at[4 + 2 * chips]),
        pltpu.make_async_copy(qg_hbm, gains_in.at[0:1], own_sem.at[5 + 2 * chips]),
        pltpu.make_async_copy(kg_hbm, gains_in.at[1:2], own_sem.at[6 + 2 * chips]),
    ]
    for copy in do_copies + own_copies + small_copies + w_copies:
        copy.start()
    pl.semaphore_wait(barrier, n + 3 * side - 3)

    order = [4, 3, 5, 2, 6, 1, 7] if n == 8 else list(range(1, n))
    arrays = ((1, k_hbm), (2, v_hbm), (0, q_hbm))

    def qkv_copy(i, ref, d, place):
        to = peer(d)
        return remote(
            ref.at[:, columns(to)],
            qkv.at[i, rows_of(place)],
            qkv_send.at[i, d],
            qkv_recv.at[i, place],
            {"seq": to},
        )

    for i, ref in arrays:
        for d in order:
            qkv_copy(i, ref, d, me).start()

    def ring(direction, step, sub, block, to):
        return remote(
            do_all.at[block, sub],
            do_all.at[block, sub],
            ag_send.at[direction, step, sub],
            ag_recv.at[block, sub],
            {"seq": to},
        )

    for copy in do_copies:
        copy.wait()
    for sub in range(SUBS):
        ring(0, 0, sub, me, up).start()
        ring(1, 0, sub, me, down).start()

    dkt[...] = jnp.zeros(dkt.shape, F32)
    dvt[...] = jnp.zeros(dvt.shape, F32)
    gain[...] = jnp.zeros(gain.shape, F32)

    def clear(i, carry):
        wacc[:, pl.ds(pl.multiple_of(i * 512, 512), 512)] = jnp.zeros((width, 512), F32)
        return carry

    lax.fori_loop(0, model // 512, clear, 0)
    for copy in small_copies:
        copy.wait()
    qg = gains_in[0:1]
    kg = gains_in[1:2]
    seg_k = seg_of(lax.broadcasted_iota(jnp.int32, (1, total), 1), lengths_ref)

    def project(t, sub):
        term = dot(do_all[t, sub], w[:, sub_of(sub)], NT)
        datt[t] = term if sub == 0 else datt[t] + term

    for copy in w_copies:
        copy.wait()
    for sub in range(SUBS):
        project(me, sub)
    for copy in own_copies:
        copy.wait()
    for i, ref in arrays:
        for d in range(1, n):
            qkv_copy(i, ref, d, peer(d)).wait_recv()

    def norm_rows(i, rows, cols):
        block = qkv[i, rows, cols].astype(F32)
        inverse = lax.rsqrt(jnp.mean(block * block, axis=-1, keepdims=True) + EPS)
        return block * inverse, inverse

    def norm_back(unit, inverse, weight, d_normed):
        d_unit = d_normed * weight
        d_rows = inverse * (d_unit - unit * jnp.mean(unit * d_unit, axis=-1, keepdims=True))
        return d_rows.astype(BF16)

    for h in range(heads):
        cols = pl.ds(h * HEAD_DIM, HEAD_DIM)

        def prepare(j, carry, cols=cols):
            rows = pl.ds(pl.multiple_of(j * 256, 256), 256)
            normed = norm_rows(1, rows, cols)[0] * kg
            kn[rows, cols] = normed.astype(BF16)
            knt[cols, rows] = jnp.transpose(normed).astype(BF16)
            vt[cols, rows] = jnp.transpose(qkv[2, rows, cols].astype(F32)).astype(BF16)
            return carry

        lax.fori_loop(0, total // 256, prepare, 0)

    def forward(j, carry):
        rows = pl.ds(pl.multiple_of(j * 256, 256), 256)
        places = lax.broadcasted_iota(jnp.int32, (256, 1), 0) + j * 256
        same = seg_of(places, lengths_ref) == seg_k
        for h in range(heads):
            cols = pl.ds(h * HEAD_DIM, HEAD_DIM)
            qn = (norm_rows(0, rows, cols)[0] * qg).astype(BF16)
            expo = jnp.where(same, jnp.exp(dot(qn, knt[cols, :]) * scale), 0.0)
            prob = (expo * (1.0 / jnp.sum(expo, axis=-1, keepdims=True))).astype(BF16)
            probs[h, rows, :] = prob
            attn = dot(prob, qkv[2, :, cols])
            attnt[cols, rows] = jnp.transpose(attn).astype(BF16)
        return carry

    lax.fori_loop(0, total // 256, forward, 0)

    def weigh(t, sub):
        def piece(j, c):
            part = pl.ds(pl.multiple_of(j * 512, 512), 512)
            into = pl.ds(pl.multiple_of(sub * quarter + j * 512, 512), 512)
            wacc[:, into] += dot(attnt[:, rows_of(t)], do_all[t, sub, :, part])
            return c

        lax.fori_loop(0, quarter // 512, piece, 0)

    def backward(t, h):
        rows = rows_of(t)
        cols = pl.ds(h * HEAD_DIM, HEAD_DIM)
        unit, inverse = norm_rows(0, rows, cols)
        normed = unit * qg
        dattn = datt[t, :, cols]
        prob = probs[h, rows, :]
        prob32 = prob.astype(F32)
        d_probs = dot(dattn.astype(BF16), vt[cols, :])
        row_sum = jnp.sum(prob32 * d_probs, axis=-1, keepdims=True)
        d_scores = (prob32 * (d_probs - row_sum) * scale).astype(BF16)
        dvt[cols, :] += dot(jnp.transpose(dattn).astype(BF16), prob)
        dkt[cols, :] += dot(jnp.transpose(normed).astype(BF16), d_scores)
        d_normed = dot(d_scores, kn[:, cols])
        gain[0:1, :] += jnp.sum(unit * d_normed, axis=0, keepdims=True)
        dqs[t, :, cols] = norm_back(unit, inverse, qg, d_normed)

    def dq_copy(t, place):
        return remote(
            dqs.at[t], dq_out.at[:, columns(place)], dq_send.at[t], dq_recv.at[place], {"seq": t}
        )

    def block_at(shift):
        return lax.rem(me + sign * shift + n, n)

    for sub in range(SUBS):
        weigh(me, sub)

    def body(step, carry):
        a_block = block_at(-step)
        b_block = block_at(step)
        a_last = block_at(1 - step)
        b_last = block_at(step - 1)
        for sub in range(SUBS):
            ring(0, step - 1, sub, a_block, up).wait_recv()
            ring(0, step, sub, a_block, up).start()
            ring(1, step - 1, sub, b_block, down).wait_recv()

            @pl.when(step < b_steps)
            def _():
                ring(1, step, sub, b_block, down).start()

            for block in (a_block, b_block):
                project(block, sub)
                weigh(block, sub)
            if sub == 0:
                backward(a_last, 0)
            elif sub == 1:
                for h in range(1, heads):
                    backward(a_last, h)
            else:

                @pl.when(step > 1)
                def _():
                    for h in (0,) if sub == 2 else range(1, heads):
                        backward(b_last, h)

        return carry

    lax.fori_loop(1, a_steps, body, 0)
    own_dq = pltpu.make_async_copy(dqs.at[me], dq_out.at[:, columns(me)], own_sem.at[0])
    own_dq.start()

    t = block_at(-a_steps)
    a_last = block_at(-b_steps)
    b_last = block_at(b_steps)

    def swap(sub):
        part = sub_of(sub)
        return remote(
            wpb.at[half_of(other), part],
            theirs.at[:, part],
            swap_send.at[sub],
            swap_recv.at[sub],
            {"dp_2": other},
        )

    def held_at(sub, place):
        return chunk_at(sub, lax.rem(sub - place + side, side)) if sub % 2 == 0 else chunk_at(sub, place)

    def first_copy(sub, d, source):
        to, place = x_peer(d) if sub % 2 == 0 else y_peer(d)
        return remote(
            packed.at[held_at(sub, place)],
            slots.at[sub, source],
            first_send.at[sub, d],
            first_recv.at[sub, source],
            to,
        )

    def first_sends(sub):
        for d in range(1, side):
            first_copy(sub, d, x if sub % 2 == 0 else y).start()

    def second_copy(sub):
        owner = lax.rem(sub - (x if sub % 2 == 0 else y) + side, side)
        source = y if sub % 2 == 0 else x
        return remote(
            part.at[sub],
            second.at[source],
            second_send.at[sub],
            second_recv.at[source],
            {"dp_0": owner} if sub % 2 == 0 else {"dp_1": owner},
        )

    def combine(sub):
        whole = packed[held_at(sub, x if sub % 2 == 0 else y)].astype(F32)
        for d in range(1, side):
            source = (x_peer(d) if sub % 2 == 0 else y_peer(d))[1]
            first_copy(sub, d, source).wait_recv()
            whole = whole + slots[sub, source].astype(F32)
        part[sub] = whole.astype(BF16)

    def second_sends(sub):
        @pl.when(home != sub)
        def _():
            second_copy(sub).start()

    def merge(sub):
        swap(sub).wait_recv()

        def piece(j, carry):
            part = chunk_of(sub * per_sub + j)
            whole = wpb[half_of(core), part].astype(F32) + theirs[:, part].astype(F32)
            packed[chunk_at(sub, j)] = whole.astype(BF16)
            return carry

        lax.fori_loop(0, per_sub, piece, 0)

    for sub in range(SUBS):
        ring(0, a_steps - 1, sub, t, up).wait_recv()
        if sub == SUBS - 1:
            for step in range(1, b_steps):
                dq_copy(block_at(-step), me).start()
                dq_copy(block_at(step), me).start()
            dq_copy(a_last, me).start()
        weigh(t, sub)

        def narrow(j, carry, sub=sub):
            part = pl.ds(pl.multiple_of(sub * quarter + j * 512, 512), 512)
            wpb[:, part] = wacc[:, part].astype(BF16)
            return carry

        lax.fori_loop(0, quarter // 512, narrow, 0)
        swap(sub).start()
        project(t, sub)
        merge(sub)
        first_sends(sub)
        if sub > 0:
            combine(sub - 1)
            second_sends(sub - 1)
        if sub < heads:
            backward(a_last, sub)
    def dkv_copy(i, h, d, place):
        to = peer(d)
        return remote(
            dkv.at[i, rows_of(to), pl.ds(h * HEAD_DIM, HEAD_DIM)],
            (dk_out, dv_out)[i].at[:, pl.ds(pl.multiple_of(place * width + h * HEAD_DIM, HEAD_DIM), HEAD_DIM)],
            dkv_send.at[i, h, d],
            dkv_recv.at[i, h, place],
            {"seq": to},
        )

    for h in range(heads):
        cols = pl.ds(h * HEAD_DIM, HEAD_DIM)
        backward(b_last, h)
        backward(t, h)

        def finish(j, carry, cols=cols):
            rows = pl.ds(pl.multiple_of(j * 256, 256), 256)
            dkv[1, rows, cols] = jnp.transpose(dvt[cols, rows]).astype(BF16)
            unit, inverse = norm_rows(1, rows, cols)
            d_normed = jnp.transpose(dkt[cols, rows])
            gain[1:2, :] += jnp.sum(unit * d_normed, axis=0, keepdims=True)
            dkv[0, rows, cols] = norm_back(unit, inverse, kg, d_normed)
            return carry

        lax.fori_loop(0, total // 256, finish, 0)
        for i in (1, 0) if h < heads - 1 else (1,):
            for d in order:
                dkv_copy(i, h, d, me).start()
        if h == 0:
            combine(SUBS - 1)
            second_sends(SUBS - 1)
    dq_copy(b_last, me).start()
    dq_copy(t, me).start()
    own_dkv = [
        pltpu.make_async_copy(dkv.at[i, rows_of(me)], out.at[:, columns(me)], own_sem.at[1 + i])
        for i, out in enumerate((dk_out, dv_out))
    ]
    for copy in own_dkv:
        copy.start()

    reduced[...] = part[home].astype(F32)
    start = jnp.where(lax.rem(home, 2) == 0, y, x)
    for d in range(1, side):
        source = lax.rem(start + d, side)
        remote(part.at[0], second.at[source], second_send.at[0], second_recv.at[source], x_peer(1)[0]).wait_recv()
        reduced[...] += second[source].astype(F32)

    def window(index):
        return pl.ds(pl.multiple_of(index * 128, 128), 256)

    shard_width = chunk // 2
    last = remote(reduced.at[:, window(other)], final, last_send.at[0], last_recv.at[0], {"dp_2": other})
    last.start()

    def pick(block):
        return jnp.where(core == 0, block[:, :shard_width], block[:, 256 - shard_width :])

    square = jnp.sum(reduced[...] * reduced[...])
    row = lax.broadcasted_iota(jnp.int32, (8, 128), 0)
    row_slots[in_row] = jnp.where(row == 2, square, gain[...])
    w_out[half_of(core), :] = pick(reduced[:, window(core)])

    def rest_of_dk():
        for d in order:
            dkv_copy(0, heads - 1, d, me).start()

    def spread(buffer, peers, count, sends, recvs, place, then=None):
        def copy(d, source):
            return remote(buffer.at[source], buffer.at[source], sends.at[d], recvs.at[source], peers(d)[0])

        for d in range(1, count):
            copy(d, place).start()
        if then is not None:
            then()
        for d in range(1, count):
            copy(d, peers(d)[1]).wait_recv()
        result = buffer[0]
        for index in range(1, count):
            result = result + buffer[index]
        for d in range(1, count):
            copy(d, place).wait_send()
        return result

    y_slots[y] = spread(row_slots, row_peer, 2 * side, row_send, row_recv, in_row)
    z_slots[me] = spread(y_slots, y_peer, side, y_send, y_recv, y)
    last.wait_recv()
    w_out[half_of(other), :] = pick(final[...])
    summed = spread(z_slots, z_peer, n, z_send, z_recv, me, rest_of_dk)
    gains = jnp.where(row < 2, summed, 0.0)
    squares = summed[2:3, 0:1] + jnp.sum(gains * gains)
    norm = jnp.sqrt(squares)
    factor = jnp.minimum(1.0, MAX_NORM / (norm + EPS))
    small_out[...] = jnp.where(row < 2, gains * factor, norm)
    w_out[...] = w_out[...] * factor
    last.wait_send()
    results = [
        pltpu.make_async_copy(small_out, small_hbm_out, own_sem.at[5 + 2 * chips]),
        pltpu.make_async_copy(w_out, w_hbm_out, own_sem.at[6 + 2 * chips]),
    ]
    for copy in results:
        copy.start()
    own_dq.wait()
    for copy in own_dkv + results:
        copy.wait()
    for i, ref in arrays:
        for d in order:
            qkv_copy(i, ref, d, me).wait_send()
    for sub in range(SUBS):
        swap(sub).wait_send()
        for step in range(a_steps):
            ring(0, step, sub, me, up).wait_send()
        for step in range(b_steps):
            ring(1, step, sub, me, down).wait_send()
        for d in range(1, side):
            first_copy(sub, d, 0).wait_send()

        @pl.when(home != sub)
        def _():
            second_copy(sub).wait_send()

    for d in range(1, n):
        dq_copy(peer(d), me).wait_send()
        dq_copy(peer(d), peer(d)).wait_recv()
        for i in (0, 1):
            for h in range(heads):
                dkv_copy(i, h, d, me).wait_send()
                dkv_copy(i, h, d, peer(d)).wait_recv()


def write_kernel(
    dq_in, dk_in, dv_in, w_in, small_in, dq_out, dk_out, dv_out, w_out, qgain_out, kgain_out, norm_out,
    rows, block, turned, small, norm, in_sem, out_sem,
):
    loads = [pltpu.make_async_copy(w_in, block, in_sem.at[0]), pltpu.make_async_copy(small_in, small, in_sem.at[1])]
    half = rows.shape[1] // 2
    pieces = [(i, pl.ds(p * half, half), 2 * i + p) for i in range(3) for p in range(2)]
    ins, outs = (dq_in, dk_in, dv_in), (dq_out, dk_out, dv_out)
    for i, part, k in pieces:
        loads.append(pltpu.make_async_copy(ins[i].at[part], rows.at[i, part], in_sem.at[2 + k]))
    for load in loads:
        load.start()
    stores = [
        pltpu.make_async_copy(small.at[0:1], qgain_out, out_sem.at[0]),
        pltpu.make_async_copy(small.at[1:2], kgain_out, out_sem.at[1]),
        pltpu.make_async_copy(norm, norm_out, out_sem.at[2]),
        pltpu.make_async_copy(turned, w_out, out_sem.at[3]),
    ]
    loads[0].wait()
    loads[1].wait()
    norm[...] = small[2:3, :]
    turned[...] = jnp.transpose(block[...])
    for store in stores:
        store.start()
    for i, part, k in pieces:
        loads[2 + k].wait()
        stores.append(pltpu.make_async_copy(rows.at[i, part], outs[i].at[part], out_sem.at[4 + k]))
        stores[-1].start()
    for store in stores:
        store.wait()


def local(n, side, query_rows, key_rows, value_rows, out_grad, clip_lengths, out_weight, query_gain, key_gain):
    tokens, inner = query_rows.shape[1:]
    model = out_grad.shape[2]
    width = inner // n
    heads = width // HEAD_DIM
    total = tokens * n
    anywhere = pl.BlockSpec(memory_space=pl.ANY)
    dma = pltpu.SemaphoreType.DMA
    struct = jax.ShapeDtypeStruct
    chips = side * side
    chunk = model // chips
    dq, dk, dv, weight_grad, small = pl.pallas_call(
        functools.partial(kernel, n, side),
        out_shape=(
            struct((tokens, inner), BF16),
            struct((tokens, inner), BF16),
            struct((tokens, inner), BF16),
            struct((width, chunk // 2), F32),
            struct((8, HEAD_DIM), F32),
        ),
        in_specs=[anywhere] * 8,
        out_specs=(anywhere,) * 5,
        scratch_shapes=[
            pltpu.SMEM(clip_lengths.shape[1:], jnp.int32),
            pltpu.VMEM((8, HEAD_DIM), F32),
            pltpu.VMEM((width, chunk // 2), F32),
            pltpu.VMEM((8, HEAD_DIM), F32),
            pltpu.VMEM((3, total, width), BF16),
            pltpu.VMEM((total, width), BF16),
            pltpu.VMEM((width, total), BF16),
            pltpu.VMEM((width, total), BF16),
            pltpu.VMEM((n, SUBS, tokens, model // SUBS), BF16),
            pltpu.VMEM((width, model), BF16),
            pltpu.VMEM((width, model), F32),
            pltpu.VMEM((width, total), F32),
            pltpu.VMEM((width, total), F32),
            pltpu.VMEM((n, tokens, width), F32),
            pltpu.VMEM((width, total), BF16),
            pltpu.VMEM((heads, total, total), BF16),
            pltpu.VMEM((n, tokens, width), BF16),
            pltpu.VMEM((2, total, width), BF16),
            pltpu.VMEM((8, HEAD_DIM), F32),
            pltpu.VMEM((width, model), BF16),
            pltpu.VMEM((width // 2, model), BF16),
            pltpu.VMEM((chips, width // 2, chunk), BF16),
            pltpu.VMEM((SUBS, side, width // 2, chunk), BF16),
            pltpu.VMEM((SUBS, width // 2, chunk), BF16),
            pltpu.VMEM((side, width // 2, chunk), BF16),
            pltpu.VMEM((width // 2, chunk), F32),
            pltpu.VMEM((width // 2, 256), F32),
            pltpu.VMEM((n, 8, 128), F32),
            pltpu.VMEM((2 * side, 8, 128), F32),
            pltpu.VMEM((side, 8, 128), F32),
            dma((3, n)),
            dma((3, n)),
            dma((2, n // 2, SUBS)),
            dma((n, SUBS)),
            dma((n,)),
            dma((n,)),
            dma((2, heads, n)),
            dma((2, heads, n)),
            dma((SUBS,)),
            dma((SUBS,)),
            dma((SUBS, side)),
            dma((SUBS, side)),
            dma((SUBS,)),
            dma((side,)),
            dma((1,)),
            dma((1,)),
            dma((n,)),
            dma((n,)),
            dma((2 * side,)),
            dma((2 * side,)),
            dma((side,)),
            dma((side,)),
            dma((7 + 2 * chips,)),
        ],
        compiler_params=pltpu.CompilerParams(
            collective_id=1, has_side_effects=True, vmem_limit_bytes=67043328
        ),
        name="fused",
    )(
        query_rows[0],
        key_rows[0],
        value_rows[0],
        out_grad[0],
        out_weight,
        clip_lengths[0],
        query_gain[None],
        key_gain[None],
    )
    rows = struct((tokens, inner), BF16)
    gain = struct((1, HEAD_DIM), F32)
    dq, dk, dv, weight_grad, qgain, kgain, norm = pl.pallas_call(
        write_kernel,
        out_shape=(rows, rows, rows, struct((chunk // 2, width), F32), gain, gain, gain),
        in_specs=[anywhere] * 5,
        out_specs=(anywhere,) * 7,
        scratch_shapes=[
            pltpu.VMEM((3, tokens, inner), BF16),
            pltpu.VMEM((width, chunk // 2), F32),
            pltpu.VMEM((chunk // 2, width), F32),
            pltpu.VMEM((8, HEAD_DIM), F32),
            pltpu.VMEM((1, HEAD_DIM), F32),
            dma((8,)),
            dma((10,)),
        ],
        name="write",
    )(dq, dk, dv, weight_grad, small)
    return (
        dq[None],
        dk[None],
        dv[None],
        weight_grad.T,
        qgain.reshape(HEAD_DIM),
        kgain.reshape(HEAD_DIM),
        norm[0, 0],
    )


def solution(mesh):
    n = mesh.shape["seq"]
    torus = Mesh(mesh.devices.reshape(4, 4, 2, n), ("dp_0", "dp_1", "dp_2", "seq"))
    return jax.shard_map(
        functools.partial(local, n, 4),
        mesh=torus,
        in_specs=(
            P(DP, "seq", None),
            P(DP, "seq", None),
            P(DP, "seq", None),
            P(DP, "seq", None),
            P(DP, None),
            P("seq", None),
            P(),
            P(),
        ),
        out_specs=(
            P(DP, "seq", None),
            P(DP, "seq", None),
            P(DP, "seq", None),
            P("seq", DP),
            P(),
            P(),
            P(),
        ),
        check_vma=False,
    )
```

```python
import functools

import jax
import jax.numpy as jnp
from jax import lax
from jax.experimental import pallas as pl
from jax.experimental.pallas import tpu as pltpu
from jax.sharding import Mesh
from jax.sharding import PartitionSpec as P

HEAD_DIM = 128
MAX_NORM = 768
EPS = 1e-06
DP = ("dp_0", "dp_1", "dp_2")
MESH = pl.DeviceIdType.MESH
F32 = jnp.float32
BF16 = jnp.bfloat16
NN = (((1,), (0,)), ((), ()))
NT = (((1,), (1,)), ((), ()))
SUBS = 4


def dot(a, b, dims=NN):
    return lax.dot_general(a, b, dims, preferred_element_type=F32)


def seg_of(places, lengths_ref):
    seg = jnp.zeros(places.shape, jnp.int32)
    end = jnp.int32(0)
    for c in range(lengths_ref.shape[0]):
        end = end + lengths_ref[c]
        seg = seg + (places >= end).astype(jnp.int32)
    return seg


def kernel(
    n,
    side,
    q_hbm,
    k_hbm,
    v_hbm,
    do_hbm,
    w_hbm,
    lengths_hbm,
    qg_hbm,
    kg_hbm,
    dq_out,
    dk_out,
    dv_out,
    w_hbm_out,
    small_hbm_out,
    lengths_ref,
    gains_in,
    w_out,
    small_out,
    qkv,
    kn,
    knt,
    vt,
    do_all,
    w,
    wacc,
    dkt,
    dvt,
    datt,
    attnt,
    probs,
    dqs,
    dkv,
    gain,
    wpb,
    theirs,
    packed,
    slots,
    part,
    second,
    reduced,
    final,
    z_slots,
    row_slots,
    y_slots,
    qkv_send,
    qkv_recv,
    ag_send,
    ag_recv,
    dq_send,
    dq_recv,
    dkv_send,
    dkv_recv,
    swap_send,
    swap_recv,
    first_send,
    first_recv,
    second_send,
    second_recv,
    last_send,
    last_recv,
    z_send,
    z_recv,
    row_send,
    row_recv,
    y_send,
    y_recv,
    own_sem,
):
    me = lax.axis_index("seq")
    y, x, core = (lax.axis_index(name) for name in DP)
    other = 1 - core
    sign = 1 - 2 * core
    tokens = q_hbm.shape[0]
    total = tokens * n
    width = q_hbm.shape[1] // n
    heads = width // HEAD_DIM
    model = do_hbm.shape[1]
    quarter = model // SUBS
    scale = HEAD_DIM ** (-0.5)
    up = lax.rem(me + sign + n, n)
    down = lax.rem(me - sign + n, n)
    a_steps = n // 2
    b_steps = n - 1 - a_steps
    chips = side * side
    chunk = model // chips
    per_sub = chips // SUBS
    half = width // 2
    in_row = x * 2 + core
    home = lax.rem(x + y, side)

    def columns(index):
        return pl.ds(pl.multiple_of(index * width, width), width)

    def rows_of(index):
        return pl.ds(pl.multiple_of(index * tokens, tokens), tokens)

    def half_of(index):
        return pl.ds(pl.multiple_of(index * half, half), half)

    def sub_of(index):
        return pl.ds(index * quarter, quarter)

    def peer(d):
        return lax.rem(me + d, n)

    def z_peer(d):
        return {"seq": peer(d)}, peer(d)

    def row_peer(d):
        place = lax.rem(in_row + d, 2 * side)
        return {"dp_1": place // 2, "dp_2": lax.rem(place, 2)}, place

    def y_peer(d):
        place = lax.rem(y + d, side)
        return {"dp_0": place}, place

    def x_peer(d):
        place = lax.rem(x + d, side)
        return {"dp_1": place}, place

    def remote(src, dst, send, recv, to):
        return pltpu.make_async_remote_copy(
            src_ref=src, dst_ref=dst, send_sem=send, recv_sem=recv, device_id=to, device_id_type=MESH
        )

    barrier = pltpu.get_barrier_semaphore()
    for d in range(1, n):
        pl.semaphore_signal(barrier, inc=1, device_id=z_peer(d)[0], device_id_type=MESH)
    for d in range(1, 2 * side):
        pl.semaphore_signal(barrier, inc=1, device_id=row_peer(d)[0], device_id_type=MESH)
    for d in range(1, side):
        pl.semaphore_signal(barrier, inc=1, device_id=y_peer(d)[0], device_id_type=MESH)

    own_copies = [
        pltpu.make_async_copy(ref.at[:, columns(me)], qkv.at[i, rows_of(me)], own_sem.at[i])
        for i, ref in enumerate((q_hbm, k_hbm, v_hbm))
    ]
    def chunk_at(sub, j):
        return side * j + lax.rem(sub - j + side, side)

    def chunk_of(index):
        return pl.ds(pl.multiple_of(index * chunk, chunk), chunk)

    do_copies = [
        pltpu.make_async_copy(
            do_hbm.at[:, chunk_of(chunk_at(sub, j))],
            do_all.at[me, sub, :, pl.ds(j * chunk, chunk)],
            own_sem.at[4 + sub * per_sub + j],
        )
        for sub in range(SUBS)
        for j in range(per_sub)
    ]
    w_copies = [
        pltpu.make_async_copy(
            w_hbm.at[:, chunk_of(chunk_at(sub, j))],
            w.at[:, pl.ds((sub * per_sub + j) * chunk, chunk)],
            own_sem.at[4 + chips + sub * per_sub + j],
        )
        for sub in range(SUBS)
        for j in range(per_sub)
    ]
    small_copies = [
        pltpu.make_async_copy(lengths_hbm, lengths_ref, own_sem.at[4 + 2 * chips]),
        pltpu.make_async_copy(qg_hbm, gains_in.at[0:1], own_sem.at[5 + 2 * chips]),
        pltpu.make_async_copy(kg_hbm, gains_in.at[1:2], own_sem.at[6 + 2 * chips]),
    ]
    for copy in do_copies + own_copies + small_copies + w_copies:
        copy.start()
    pl.semaphore_wait(barrier, n + 3 * side - 3)

    order = [4, 3, 5, 2, 6, 1, 7] if n == 8 else list(range(1, n))
    arrays = ((1, k_hbm), (2, v_hbm), (0, q_hbm))

    def qkv_copy(i, ref, d, place):
        to = peer(d)
        return remote(
            ref.at[:, columns(to)],
            qkv.at[i, rows_of(place)],
            qkv_send.at[i, d],
            qkv_recv.at[i, place],
            {"seq": to},
        )

    for i, ref in arrays:
        for d in order:
            qkv_copy(i, ref, d, me).start()

    def ring(direction, step, sub, block, to):
        return remote(
            do_all.at[block, sub],
            do_all.at[block, sub],
            ag_send.at[direction, step, sub],
            ag_recv.at[block, sub],
            {"seq": to},
        )

    for copy in do_copies:
        copy.wait()
    for sub in range(SUBS):
        ring(0, 0, sub, me, up).start()
        ring(1, 0, sub, me, down).start()

    dkt[...] = jnp.zeros(dkt.shape, F32)
    dvt[...] = jnp.zeros(dvt.shape, F32)
    gain[...] = jnp.zeros(gain.shape, F32)

    def clear(i, carry):
        wacc[:, pl.ds(pl.multiple_of(i * 512, 512), 512)] = jnp.zeros((width, 512), F32)
        return carry

    lax.fori_loop(0, model // 512, clear, 0)
    for copy in small_copies:
        copy.wait()
    qg = gains_in[0:1]
    kg = gains_in[1:2]
    seg_k = seg_of(lax.broadcasted_iota(jnp.int32, (1, total), 1), lengths_ref)

    def project(t, sub):
        term = dot(do_all[t, sub], w[:, sub_of(sub)], NT)
        datt[t] = term if sub == 0 else datt[t] + term

    for copy in w_copies:
        copy.wait()
    for sub in range(SUBS):
        project(me, sub)
    for copy in own_copies:
        copy.wait()
    for i, ref in arrays:
        for d in range(1, n):
            qkv_copy(i, ref, d, peer(d)).wait_recv()

    def norm_rows(i, rows, cols):
        block = qkv[i, rows, cols].astype(F32)
        inverse = lax.rsqrt(jnp.mean(block * block, axis=-1, keepdims=True) + EPS)
        return block * inverse, inverse

    def norm_back(unit, inverse, weight, d_normed):
        d_unit = d_normed * weight
        d_rows = inverse * (d_unit - unit * jnp.mean(unit * d_unit, axis=-1, keepdims=True))
        return d_rows.astype(BF16)

    for h in range(heads):
        cols = pl.ds(h * HEAD_DIM, HEAD_DIM)

        def prepare(j, carry, cols=cols):
            rows = pl.ds(pl.multiple_of(j * 256, 256), 256)
            normed = norm_rows(1, rows, cols)[0] * kg
            kn[rows, cols] = normed.astype(BF16)
            knt[cols, rows] = jnp.transpose(normed).astype(BF16)
            vt[cols, rows] = jnp.transpose(qkv[2, rows, cols].astype(F32)).astype(BF16)
            return carry

        lax.fori_loop(0, total // 256, prepare, 0)

    def forward(j, carry):
        rows = pl.ds(pl.multiple_of(j * 256, 256), 256)
        places = lax.broadcasted_iota(jnp.int32, (256, 1), 0) + j * 256
        same = seg_of(places, lengths_ref) == seg_k
        for h in range(heads):
            cols = pl.ds(h * HEAD_DIM, HEAD_DIM)
            qn = (norm_rows(0, rows, cols)[0] * qg).astype(BF16)
            expo = jnp.where(same, jnp.exp(dot(qn, knt[cols, :]) * scale), 0.0)
            prob = (expo * (1.0 / jnp.sum(expo, axis=-1, keepdims=True))).astype(BF16)
            probs[h, rows, :] = prob
            attn = dot(prob, qkv[2, :, cols])
            attnt[cols, rows] = jnp.transpose(attn).astype(BF16)
        return carry

    lax.fori_loop(0, total // 256, forward, 0)

    def weigh(t, sub):
        def piece(j, c):
            part = pl.ds(pl.multiple_of(j * 512, 512), 512)
            into = pl.ds(pl.multiple_of(sub * quarter + j * 512, 512), 512)
            wacc[:, into] += dot(attnt[:, rows_of(t)], do_all[t, sub, :, part])
            return c

        lax.fori_loop(0, quarter // 512, piece, 0)

    def backward(t, h):
        rows = rows_of(t)
        cols = pl.ds(h * HEAD_DIM, HEAD_DIM)
        unit, inverse = norm_rows(0, rows, cols)
        normed = unit * qg
        dattn = datt[t, :, cols]
        prob = probs[h, rows, :]
        prob32 = prob.astype(F32)
        d_probs = dot(dattn.astype(BF16), vt[cols, :])
        row_sum = jnp.sum(prob32 * d_probs, axis=-1, keepdims=True)
        d_scores = (prob32 * (d_probs - row_sum) * scale).astype(BF16)
        dvt[cols, :] += dot(jnp.transpose(dattn).astype(BF16), prob)
        dkt[cols, :] += dot(jnp.transpose(normed).astype(BF16), d_scores)
        d_normed = dot(d_scores, kn[:, cols])
        gain[0:1, :] += jnp.sum(unit * d_normed, axis=0, keepdims=True)
        dqs[t, :, cols] = norm_back(unit, inverse, qg, d_normed)

    def dq_copy(t, place):
        return remote(
            dqs.at[t], dq_out.at[:, columns(place)], dq_send.at[t], dq_recv.at[place], {"seq": t}
        )

    def block_at(shift):
        return lax.rem(me + sign * shift + n, n)

    for sub in range(SUBS):
        weigh(me, sub)

    def body(step, carry):
        a_block = block_at(-step)
        b_block = block_at(step)
        a_last = block_at(1 - step)
        b_last = block_at(step - 1)
        for sub in range(SUBS):
            ring(0, step - 1, sub, a_block, up).wait_recv()
            ring(0, step, sub, a_block, up).start()
            ring(1, step - 1, sub, b_block, down).wait_recv()

            @pl.when(step < b_steps)
            def _():
                ring(1, step, sub, b_block, down).start()

            for block in (a_block, b_block):
                project(block, sub)
                weigh(block, sub)
            if sub == 0:
                backward(a_last, 0)
            elif sub == 1:
                for h in range(1, heads):
                    backward(a_last, h)
            else:

                @pl.when(step > 1)
                def _():
                    for h in (0,) if sub == 2 else range(1, heads):
                        backward(b_last, h)

        return carry

    lax.fori_loop(1, a_steps, body, 0)
    own_dq = pltpu.make_async_copy(dqs.at[me], dq_out.at[:, columns(me)], own_sem.at[0])
    own_dq.start()

    t = block_at(-a_steps)
    a_last = block_at(-b_steps)
    b_last = block_at(b_steps)

    def swap(sub):
        part = sub_of(sub)
        return remote(
            wpb.at[half_of(other), part],
            theirs.at[:, part],
            swap_send.at[sub],
            swap_recv.at[sub],
            {"dp_2": other},
        )

    def held_at(sub, place):
        return chunk_at(sub, lax.rem(sub - place + side, side)) if sub % 2 == 0 else chunk_at(sub, place)

    def first_copy(sub, d, source):
        to, place = x_peer(d) if sub % 2 == 0 else y_peer(d)
        return remote(
            packed.at[held_at(sub, place)],
            slots.at[sub, source],
            first_send.at[sub, d],
            first_recv.at[sub, source],
            to,
        )

    def first_sends(sub):
        for d in range(1, side):
            first_copy(sub, d, x if sub % 2 == 0 else y).start()

    def second_copy(sub):
        owner = lax.rem(sub - (x if sub % 2 == 0 else y) + side, side)
        source = y if sub % 2 == 0 else x
        return remote(
            part.at[sub],
            second.at[source],
            second_send.at[sub],
            second_recv.at[source],
            {"dp_0": owner} if sub % 2 == 0 else {"dp_1": owner},
        )

    def combine(sub):
        whole = packed[held_at(sub, x if sub % 2 == 0 else y)].astype(F32)
        for d in range(1, side):
            source = (x_peer(d) if sub % 2 == 0 else y_peer(d))[1]
            first_copy(sub, d, source).wait_recv()
            whole = whole + slots[sub, source].astype(F32)
        part[sub] = whole.astype(BF16)

    def second_sends(sub):
        @pl.when(home != sub)
        def _():
            second_copy(sub).start()

    def merge(sub):
        swap(sub).wait_recv()

        def piece(j, carry):
            part = chunk_of(sub * per_sub + j)
            whole = wpb[half_of(core), part].astype(F32) + theirs[:, part].astype(F32)
            packed[chunk_at(sub, j)] = whole.astype(BF16)
            return carry

        lax.fori_loop(0, per_sub, piece, 0)

    for sub in range(SUBS):
        ring(0, a_steps - 1, sub, t, up).wait_recv()
        if sub == SUBS - 1:
            for step in range(1, b_steps):
                dq_copy(block_at(-step), me).start()
                dq_copy(block_at(step), me).start()
            dq_copy(a_last, me).start()
        weigh(t, sub)

        def narrow(j, carry, sub=sub):
            part = pl.ds(pl.multiple_of(sub * quarter + j * 512, 512), 512)
            wpb[:, part] = wacc[:, part].astype(BF16)
            return carry

        lax.fori_loop(0, quarter // 512, narrow, 0)
        swap(sub).start()
        project(t, sub)
        merge(sub)
        first_sends(sub)
        if 0 < sub < SUBS - 1:
            combine(sub - 1)
            second_sends(sub - 1)
        if sub < heads:
            backward(a_last, sub)
    def dkv_copy(i, h, d, place):
        to = peer(d)
        return remote(
            dkv.at[i, rows_of(to), pl.ds(h * HEAD_DIM, HEAD_DIM)],
            (dk_out, dv_out)[i].at[:, pl.ds(pl.multiple_of(place * width + h * HEAD_DIM, HEAD_DIM), HEAD_DIM)],
            dkv_send.at[i, h, d],
            dkv_recv.at[i, h, place],
            {"seq": to},
        )

    for h in range(heads):
        cols = pl.ds(h * HEAD_DIM, HEAD_DIM)
        backward(b_last, h)
        backward(t, h)

        def finish(j, carry, cols=cols):
            rows = pl.ds(pl.multiple_of(j * 256, 256), 256)
            dkv[1, rows, cols] = jnp.transpose(dvt[cols, rows]).astype(BF16)
            unit, inverse = norm_rows(1, rows, cols)
            d_normed = jnp.transpose(dkt[cols, rows])
            gain[1:2, :] += jnp.sum(unit * d_normed, axis=0, keepdims=True)
            dkv[0, rows, cols] = norm_back(unit, inverse, kg, d_normed)
            return carry

        lax.fori_loop(0, total // 256, finish, 0)
        for i in (1, 0) if h < heads - 1 else (1,):
            for d in order:
                dkv_copy(i, h, d, me).start()
        if h == 0:
            for sub in (SUBS - 2, SUBS - 1):
                combine(sub)
                second_sends(sub)
    dq_copy(b_last, me).start()
    dq_copy(t, me).start()
    own_dkv = [
        pltpu.make_async_copy(dkv.at[i, rows_of(me)], out.at[:, columns(me)], own_sem.at[1 + i])
        for i, out in enumerate((dk_out, dv_out))
    ]
    for copy in own_dkv:
        copy.start()

    reduced[...] = part[home].astype(F32)
    start = jnp.where(lax.rem(home, 2) == 0, y, x)
    for d in range(1, side):
        source = lax.rem(start + d, side)
        remote(part.at[0], second.at[source], second_send.at[0], second_recv.at[source], x_peer(1)[0]).wait_recv()
        reduced[...] += second[source].astype(F32)

    def window(index):
        return pl.ds(pl.multiple_of(index * 128, 128), 256)

    shard_width = chunk // 2
    last = remote(reduced.at[:, window(other)], final, last_send.at[0], last_recv.at[0], {"dp_2": other})
    last.start()

    def pick(block):
        return jnp.where(core == 0, block[:, :shard_width], block[:, 256 - shard_width :])

    square = jnp.sum(reduced[...] * reduced[...])
    row = lax.broadcasted_iota(jnp.int32, (8, 128), 0)
    row_slots[in_row] = jnp.where(row == 2, square, gain[...])
    w_out[half_of(core), :] = pick(reduced[:, window(core)])

    def rest_of_dk():
        for d in order:
            dkv_copy(0, heads - 1, d, me).start()

    def spread(buffer, peers, count, sends, recvs, place, then=None):
        def copy(d, source):
            return remote(buffer.at[source], buffer.at[source], sends.at[d], recvs.at[source], peers(d)[0])

        for d in range(1, count):
            copy(d, place).start()
        if then is not None:
            then()
        for d in range(1, count):
            copy(d, peers(d)[1]).wait_recv()
        result = buffer[0]
        for index in range(1, count):
            result = result + buffer[index]
        for d in range(1, count):
            copy(d, place).wait_send()
        return result

    y_slots[y] = spread(row_slots, row_peer, 2 * side, row_send, row_recv, in_row)
    z_slots[me] = spread(y_slots, y_peer, side, y_send, y_recv, y)
    last.wait_recv()
    w_out[half_of(other), :] = pick(final[...])
    summed = spread(z_slots, z_peer, n, z_send, z_recv, me, rest_of_dk)
    gains = jnp.where(row < 2, summed, 0.0)
    squares = summed[2:3, 0:1] + jnp.sum(gains * gains)
    norm = jnp.sqrt(squares)
    factor = jnp.minimum(1.0, MAX_NORM / (norm + EPS))
    small_out[...] = jnp.where(row < 2, gains * factor, norm)
    w_out[...] = w_out[...] * factor
    last.wait_send()
    results = [
        pltpu.make_async_copy(small_out, small_hbm_out, own_sem.at[5 + 2 * chips]),
        pltpu.make_async_copy(w_out, w_hbm_out, own_sem.at[6 + 2 * chips]),
    ]
    for copy in results:
        copy.start()
    own_dq.wait()
    for copy in own_dkv + results:
        copy.wait()
    for i, ref in arrays:
        for d in order:
            qkv_copy(i, ref, d, me).wait_send()
    for sub in range(SUBS):
        swap(sub).wait_send()
        for step in range(a_steps):
            ring(0, step, sub, me, up).wait_send()
        for step in range(b_steps):
            ring(1, step, sub, me, down).wait_send()
        for d in range(1, side):
            first_copy(sub, d, 0).wait_send()

        @pl.when(home != sub)
        def _():
            second_copy(sub).wait_send()

    for d in range(1, n):
        dq_copy(peer(d), me).wait_send()
        dq_copy(peer(d), peer(d)).wait_recv()
        for i in (0, 1):
            for h in range(heads):
                dkv_copy(i, h, d, me).wait_send()
                dkv_copy(i, h, d, peer(d)).wait_recv()


def write_kernel(
    dq_in, dk_in, dv_in, w_in, small_in, dq_out, dk_out, dv_out, w_out, qgain_out, kgain_out, norm_out,
    rows, block, turned, small, norm, in_sem, out_sem,
):
    loads = [pltpu.make_async_copy(w_in, block, in_sem.at[0]), pltpu.make_async_copy(small_in, small, in_sem.at[1])]
    half = rows.shape[1] // 2
    pieces = [(i, pl.ds(p * half, half), 2 * i + p) for i in range(3) for p in range(2)]
    ins, outs = (dq_in, dk_in, dv_in), (dq_out, dk_out, dv_out)
    for i, part, k in pieces:
        loads.append(pltpu.make_async_copy(ins[i].at[part], rows.at[i, part], in_sem.at[2 + k]))
    for load in loads:
        load.start()
    stores = [
        pltpu.make_async_copy(small.at[0:1], qgain_out, out_sem.at[0]),
        pltpu.make_async_copy(small.at[1:2], kgain_out, out_sem.at[1]),
        pltpu.make_async_copy(norm, norm_out, out_sem.at[2]),
        pltpu.make_async_copy(turned, w_out, out_sem.at[3]),
    ]
    small_stores = list(stores)
    for i, part, k in pieces[:2]:
        loads[2 + k].wait()
        stores.append(pltpu.make_async_copy(rows.at[i, part], outs[i].at[part], out_sem.at[4 + k]))
        stores[-1].start()
    loads[0].wait()
    loads[1].wait()
    norm[...] = small[2:3, :]
    turned[...] = jnp.transpose(block[...])
    for store in small_stores:
        store.start()
    for i, part, k in pieces[2:]:
        loads[2 + k].wait()
        stores.append(pltpu.make_async_copy(rows.at[i, part], outs[i].at[part], out_sem.at[4 + k]))
        stores[-1].start()
    for store in stores:
        store.wait()


def local(n, side, query_rows, key_rows, value_rows, out_grad, clip_lengths, out_weight, query_gain, key_gain):
    tokens, inner = query_rows.shape[1:]
    model = out_grad.shape[2]
    width = inner // n
    heads = width // HEAD_DIM
    total = tokens * n
    anywhere = pl.BlockSpec(memory_space=pl.ANY)
    dma = pltpu.SemaphoreType.DMA
    struct = jax.ShapeDtypeStruct
    chips = side * side
    chunk = model // chips
    dq, dk, dv, weight_grad, small = pl.pallas_call(
        functools.partial(kernel, n, side),
        out_shape=(
            struct((tokens, inner), BF16),
            struct((tokens, inner), BF16),
            struct((tokens, inner), BF16),
            struct((width, chunk // 2), F32),
            struct((8, HEAD_DIM), F32),
        ),
        in_specs=[anywhere] * 8,
        out_specs=(anywhere,) * 5,
        scratch_shapes=[
            pltpu.SMEM(clip_lengths.shape[1:], jnp.int32),
            pltpu.VMEM((8, HEAD_DIM), F32),
            pltpu.VMEM((width, chunk // 2), F32),
            pltpu.VMEM((8, HEAD_DIM), F32),
            pltpu.VMEM((3, total, width), BF16),
            pltpu.VMEM((total, width), BF16),
            pltpu.VMEM((width, total), BF16),
            pltpu.VMEM((width, total), BF16),
            pltpu.VMEM((n, SUBS, tokens, model // SUBS), BF16),
            pltpu.VMEM((width, model), BF16),
            pltpu.VMEM((width, model), F32),
            pltpu.VMEM((width, total), F32),
            pltpu.VMEM((width, total), F32),
            pltpu.VMEM((n, tokens, width), F32),
            pltpu.VMEM((width, total), BF16),
            pltpu.VMEM((heads, total, total), BF16),
            pltpu.VMEM((n, tokens, width), BF16),
            pltpu.VMEM((2, total, width), BF16),
            pltpu.VMEM((8, HEAD_DIM), F32),
            pltpu.VMEM((width, model), BF16),
            pltpu.VMEM((width // 2, model), BF16),
            pltpu.VMEM((chips, width // 2, chunk), BF16),
            pltpu.VMEM((SUBS, side, width // 2, chunk), BF16),
            pltpu.VMEM((SUBS, width // 2, chunk), BF16),
            pltpu.VMEM((side, width // 2, chunk), BF16),
            pltpu.VMEM((width // 2, chunk), F32),
            pltpu.VMEM((width // 2, 256), F32),
            pltpu.VMEM((n, 8, 128), F32),
            pltpu.VMEM((2 * side, 8, 128), F32),
            pltpu.VMEM((side, 8, 128), F32),
            dma((3, n)),
            dma((3, n)),
            dma((2, n // 2, SUBS)),
            dma((n, SUBS)),
            dma((n,)),
            dma((n,)),
            dma((2, heads, n)),
            dma((2, heads, n)),
            dma((SUBS,)),
            dma((SUBS,)),
            dma((SUBS, side)),
            dma((SUBS, side)),
            dma((SUBS,)),
            dma((side,)),
            dma((1,)),
            dma((1,)),
            dma((n,)),
            dma((n,)),
            dma((2 * side,)),
            dma((2 * side,)),
            dma((side,)),
            dma((side,)),
            dma((7 + 2 * chips,)),
        ],
        compiler_params=pltpu.CompilerParams(
            collective_id=1, has_side_effects=True, vmem_limit_bytes=67043328
        ),
        name="fused",
    )(
        query_rows[0],
        key_rows[0],
        value_rows[0],
        out_grad[0],
        out_weight,
        clip_lengths[0],
        query_gain[None],
        key_gain[None],
    )
    rows = struct((tokens, inner), BF16)
    gain = struct((1, HEAD_DIM), F32)
    dq, dk, dv, weight_grad, qgain, kgain, norm = pl.pallas_call(
        write_kernel,
        out_shape=(rows, rows, rows, struct((chunk // 2, width), F32), gain, gain, gain),
        in_specs=[anywhere] * 5,
        out_specs=(anywhere,) * 7,
        scratch_shapes=[
            pltpu.VMEM((3, tokens, inner), BF16),
            pltpu.VMEM((width, chunk // 2), F32),
            pltpu.VMEM((chunk // 2, width), F32),
            pltpu.VMEM((8, HEAD_DIM), F32),
            pltpu.VMEM((1, HEAD_DIM), F32),
            dma((8,)),
            dma((10,)),
        ],
        name="write",
    )(dq, dk, dv, weight_grad, small)
    return (
        dq[None],
        dk[None],
        dv[None],
        weight_grad.T,
        qgain.reshape(HEAD_DIM),
        kgain.reshape(HEAD_DIM),
        norm[0, 0],
    )


def solution(mesh):
    n = mesh.shape["seq"]
    torus = Mesh(mesh.devices.reshape(4, 4, 2, n), ("dp_0", "dp_1", "dp_2", "seq"))
    return jax.shard_map(
        functools.partial(local, n, 4),
        mesh=torus,
        in_specs=(
            P(DP, "seq", None),
            P(DP, "seq", None),
            P(DP, "seq", None),
            P(DP, "seq", None),
            P(DP, None),
            P("seq", None),
            P(),
            P(),
        ),
        out_specs=(
            P(DP, "seq", None),
            P(DP, "seq", None),
            P(DP, "seq", None),
            P("seq", DP),
            P(),
            P(),
            P(),
        ),
        check_vma=False,
    )
```
